32 devices in a mesh: member: 2 (over y), tile: 4 (over z), lev: 2 (over x), sub: 2 (over core).
Axes of the slice: x: 2, y: 2, z: 4, core: 2. Of those that a mesh axis runs over, the one named last changes fastest.
Arguments:
- increment: float32 [4, 1024, 128], P(('member', 'lev'), ('tile', 'sub')), parts along dimension 0, may hold values from -6 to 6
- residual: float32 [4, 1024, 128], P(('member', 'lev'), ('tile', 'sub')), parts along dimension 0, may hold values from -6 to 6
- direction: float32 [4, 1024, 128], P(('member', 'lev'), ('tile', 'sub')), parts along dimension 0, may hold values from -6 to 6
- wind_u: bfloat16 [4, 1024, 128], P(('member', 'lev'), ('tile', 'sub')), parts along dimension 0, may hold values from -0.3984375 to 0.3984375
- wind_v: bfloat16 [4, 1024, 128], P(('member', 'lev'), ('tile', 'sub')), parts along dimension 0, may hold values from -0.3984375 to 0.3984375
- diffusion: float32 [2], replicated, may hold values from 0.03 to 0.12
- vertical: float32 [2], replicated, may hold values from 0.02 to 0.1
- background_inv: float32 [2], replicated, may hold values from 0.5 to 2
- side_pair: int32 [8, 4], replicated, may hold values from 0 to 31, as said below
- side_flip: int32 [8, 4], replicated, may hold values from 0 to 1, as said below
- obs_column: int32 [512], P(('tile', 'sub')), may hold values from 0 to 131071, as said below
- obs_time: int32 [512], P(('tile', 'sub')), may hold values from 1 to 4
- obs_count: int32 [8], P(('tile', 'sub')), may hold values from 48 to 64, as said below
- jacobian: bfloat16 [512, 2, 616], P(('tile', 'sub'), 'lev'), may hold values from -4 to 4
- error_inv: float32 [616], replicated, may hold values from 0.2 to 5
Outputs:
- increment_new: float32 [4, 1024, 128], P(('member', 'lev'), ('tile', 'sub')), parts along dimension 0
- residual_new: float32 [4, 1024, 128], P(('member', 'lev'), ('tile', 'sub')), parts along dimension 0
- direction_new: float32 [4, 1024, 128], P(('member', 'lev'), ('tile', 'sub')), parts along dimension 0
The draws below stay inside these ranges and needn't reach their ends.
There are 2 independent parts, one for each index of `member`. The reference program is written for one: setup_inputs(seed, part) draws one part's arguments, and reference() takes and returns one part's arrays. A program takes and returns all parts, laid end to end along the dimension named above; an argument that names none is the same for every part. Nothing has to cross between parts.
Inputs may be any that keep to these rules, and one draw needn't show every extreme that they name: side_pair[side_pair[k]] == k for every side k, and side_pair[k] is a side of another panel, so the panels close into one surface joined edge to edge. side_flip is equal on both sides of a pair. `obs_column`: among the live slots of one owner at most 16 name columns of one panel, and every owner reaches 16 for some panel. `obs_count`: some owner has all 64 slots live.
All inputs are finite; a program needn't handle non-finite values.
Results may differ from the reference program's by a relative error of at most 0.0003.
Values sent between devices are 32-bit elements; how exact they have to be, the bound alone decides.
A program may use at most 64 MiB of HBM per device.

```python
import math
import jax
import jax.numpy as jnp
from jax import lax

W = 128
STEPS = 4
CH = 616
OBS_DEV = 64
PANELS = 8
LEVELS = 2
NOBS = 512
CAP = 16


def side_pairing(key):
    inner = jax.random.fold_in(key, 7)
    first_key, second_key = jax.random.split(inner)
    order = jax.random.permutation(first_key, PANELS).astype(jnp.int32)
    stride = 1 + PANELS // 8
    places = jnp.arange(PANELS, dtype=jnp.int32)
    below = order[(places + 1) % PANELS]
    beside = order[(places + stride) % PANELS]
    lower_sides = 4 * order + 1
    upper_sides = 4 * below + 0
    east_sides = 4 * order + 3
    west_sides = 4 * beside + 2
    leading = jnp.concatenate([lower_sides, east_sides]).astype(jnp.int32)
    trailing = jnp.concatenate([upper_sides, west_sides]).astype(jnp.int32)
    paired = jnp.zeros((4 * PANELS,), jnp.int32).at[leading].set(trailing).at[trailing].set(leading)
    bits = jax.random.randint(second_key, (2 * PANELS,), 0, 2).astype(jnp.int32)
    flipped = jnp.zeros((4 * PANELS,), jnp.int32).at[leading].set(bits).at[trailing].set(bits)
    return (paired.reshape(PANELS, 4), flipped.reshape(PANELS, 4))


def draw_side_pair(key, part):
    return side_pairing(key)[0]


def draw_side_flip(key, part):
    return side_pairing(key)[1]


def draw_obs_column(key, part):
    inner = jax.random.fold_in(key, 11)

    def one_owner(owner_key):
        perm_key, shuffle_key, cell_key = jax.random.split(owner_key, 3)
        order = jax.random.permutation(perm_key, PANELS).astype(jnp.int32)
        others = jax.random.permutation(shuffle_key, jnp.repeat(order[1:], CAP))
        targets = jnp.concatenate([jnp.full((CAP,), order[0], jnp.int32), others.astype(jnp.int32)])[:OBS_DEV]
        cells = jax.random.randint(cell_key, (OBS_DEV,), 0, W * W).astype(jnp.int32)
        return targets * (W * W) + cells
    return jax.vmap(one_owner)(jax.random.split(inner, PANELS)).reshape(PANELS * OBS_DEV).astype(jnp.int32)


def draw_obs_count(key, part):
    inner = jax.random.fold_in(key, 13)
    count_key, pick_key = jax.random.split(inner)
    counts = jax.random.randint(count_key, (PANELS,), (3 * OBS_DEV + 3) // 4, OBS_DEV + 1).astype(jnp.int32)
    chosen = jax.random.randint(pick_key, (), 0, PANELS)
    return counts.at[chosen].set(OBS_DEV)


def set_ends(result, key, smallest, high):
    dims = result.shape
    place = [jax.random.randint(jax.random.fold_in(key, axis), (), 0, dims[axis]) for axis in range(len(dims))]
    result = result.at[tuple(place)].set(smallest)
    longest = dims.index(max(dims))
    place[longest] = (place[longest] + 1) % dims[longest]
    return result.at[tuple(place)].set(high)


def level_of(stream_key, extent, cuts, smallest, top_value):
    def one(position, shards_of):
        steps = jax.random.uniform(jax.random.fold_in(jax.random.fold_in(stream_key, 6), position), (shards_of,), jnp.float32, smallest / len(cuts), top_value / len(cuts))
        return jnp.repeat(jnp.exp(steps), extent[position] // shards_of).reshape((-1,) + (1,) * (len(extent) - position - 1))

    factor_of = one(*cuts[0])
    for cut in cuts[1:]:
        factor_of = factor_of * one(*cut)
    return factor_of


def scatter_about(key, extent, scale, bound, pieces=(), held_as=jnp.bfloat16):
    entries = scale * jax.random.normal(key, extent, jnp.float32)
    if pieces:
        entries = entries * level_of(key, extent, pieces, -0.22, 0.18)
    return jnp.clip(entries, -bound, bound).astype(held_as)


def setup_inputs(seed: int = 0, part: int = 0) -> dict:
    key_list = jax.random.split(jax.random.key(seed), 16)
    part_keys = jax.random.split(jax.random.fold_in(key_list[15], part), 16)
    return {
        "increment": scatter_about(part_keys[0], (LEVELS, PANELS * W, W), 1.0, 6.0, ((0, 2), (1, 8)), jnp.float32),
        "residual": scatter_about(part_keys[1], (LEVELS, PANELS * W, W), 1.0, 6.0, ((0, 2), (1, 8)), jnp.float32),
        "direction": scatter_about(part_keys[2], (LEVELS, PANELS * W, W), 1.0, 6.0, ((0, 2), (1, 8)), jnp.float32),
        "wind_u": jnp.clip(jax.random.uniform(part_keys[3], (LEVELS, PANELS * W, W), jnp.float32, -0.3984375, 0.3984375) * level_of(part_keys[3], (LEVELS, PANELS * W, W), ((0, 2), (1, 8)), -0.4, 0.0), -0.3984375, 0.3984375).astype(jnp.bfloat16),
        "wind_v": jnp.clip(jax.random.uniform(part_keys[4], (LEVELS, PANELS * W, W), jnp.float32, -0.3984375, 0.3984375) * level_of(part_keys[4], (LEVELS, PANELS * W, W), ((0, 2), (1, 8)), -0.4, 0.0), -0.3984375, 0.3984375).astype(jnp.bfloat16),
        "diffusion": jnp.clip(jnp.exp(jax.random.uniform(key_list[5], (LEVELS,), jnp.float32, math.log(0.03), math.log(0.12))), 0.03, 0.12),
        "vertical": jnp.clip(jnp.exp(jax.random.uniform(key_list[6], (LEVELS,), jnp.float32, math.log(0.02), math.log(0.1))), 0.02, 0.1),
        "background_inv": jnp.clip(jnp.exp(jax.random.uniform(key_list[7], (LEVELS,), jnp.float32, math.log(0.5), math.log(2.0))), 0.5, 2.0),
        "side_pair": draw_side_pair(jax.random.fold_in(key_list[15], 71), part),
        "side_flip": draw_side_flip(jax.random.fold_in(key_list[15], 71), part),
        "obs_column": draw_obs_column(jax.random.fold_in(key_list[15], 71), part),
        "obs_time": set_ends(jax.random.randint(key_list[11], (NOBS,), 1, STEPS + 1), jax.random.fold_in(key_list[11], 1), 1, STEPS).astype(jnp.int32),
        "obs_count": draw_obs_count(jax.random.fold_in(key_list[15], 71), part),
        "jacobian": scatter_about(key_list[13], (NOBS, LEVELS, CH), LEVELS ** -0.5, 4.0, ((0, 8), (1, 2))),
        "error_inv": jnp.clip(jnp.exp(jax.random.uniform(key_list[14], (CH,), jnp.float32, math.log(0.2), math.log(5.0))), 0.2, 5.0),
    }


def edge_strips(field):
    stacked = jnp.stack([field[:, :, 0, :], field[:, :, -1, :], field[:, :, :, 0], field[:, :, :, -1]], axis=0)
    return jnp.transpose(stacked, (2, 0, 1, 3)).reshape(PANELS * 4, LEVELS, W)


def neighbour_strips(strips, side_pair, side_flip):
    picked = strips[side_pair]
    picked = jnp.where(side_flip[:, :, None, None] == 1, picked[:, :, :, ::-1], picked)
    return jnp.transpose(picked, (1, 2, 0, 3))


def coefficients(wind_u, wind_v, diffusion, vertical):
    speed_u = wind_u.astype(jnp.float32).reshape(LEVELS, PANELS, W, W)
    speed_v = wind_v.astype(jnp.float32).reshape(LEVELS, PANELS, W, W)
    mixing = diffusion[:, None, None, None]
    coefs = (mixing + 0.5 * speed_u, mixing - 0.5 * speed_u, mixing + 0.5 * speed_v, mixing - 0.5 * speed_v)
    center = (1.0 - 4.0 * diffusion - 2.0 * vertical)[:, None, None, None]
    return coefs, center


def forward_step(field, coefs, center, vertical, side_pair, side_flip):
    halos = neighbour_strips(edge_strips(field), side_pair, side_flip)
    north = jnp.concatenate([halos[0][:, :, None, :], field[:, :, :-1, :]], axis=2)
    south = jnp.concatenate([field[:, :, 1:, :], halos[1][:, :, None, :]], axis=2)
    west = jnp.concatenate([halos[2][:, :, :, None], field[:, :, :, :-1]], axis=3)
    east = jnp.concatenate([field[:, :, :, 1:], halos[3][:, :, :, None]], axis=3)
    padded = jnp.pad(field, ((1, 1), (0, 0), (0, 0), (0, 0)))
    mixing = vertical[:, None, None, None] * (padded[:-2] + padded[2:])
    return center * field + coefs[0] * north + coefs[1] * south + coefs[2] * west + coefs[3] * east + mixing


def adjoint_step(field, coefs, center, vertical, side_pair, side_flip):
    prods = [c * field for c in coefs]
    strips = jnp.stack([prods[0][:, :, 0, :], prods[1][:, :, -1, :], prods[2][:, :, :, 0], prods[3][:, :, :, -1]], axis=0)
    strips = jnp.transpose(strips, (2, 0, 1, 3)).reshape(PANELS * 4, LEVELS, W)
    halos = neighbour_strips(strips, side_pair, side_flip)
    rows_term = jnp.concatenate([prods[0][:, :, 1:, :], halos[1][:, :, None, :]], axis=2)
    rows_term = rows_term + jnp.concatenate([halos[0][:, :, None, :], prods[1][:, :, :-1, :]], axis=2)
    cols_term = jnp.concatenate([prods[2][:, :, :, 1:], halos[3][:, :, :, None]], axis=3)
    cols_term = cols_term + jnp.concatenate([halos[2][:, :, :, None], prods[3][:, :, :, :-1]], axis=3)
    padded = jnp.pad(vertical[:, None, None, None] * field, ((1, 1), (0, 0), (0, 0), (0, 0)))
    return center * field + rows_term + cols_term + padded[:-2] + padded[2:]


def reference(increment, residual, direction, wind_u, wind_v, diffusion, vertical, background_inv, side_pair, side_flip, obs_column, obs_time, obs_count, jacobian, error_inv):
    coefs, center = coefficients(wind_u, wind_v, diffusion, vertical)
    state = direction.reshape(LEVELS, PANELS, W, W)
    states = []
    for step in range(STEPS):
        state = forward_step(state, coefs, center, vertical, side_pair, side_flip)
        states.append(state.reshape(LEVELS, PANELS * W * W))
    history = jnp.stack(states, axis=0)
    earlier = (obs_time - 1).astype(jnp.int32)
    columns = history[earlier, :, obs_column]
    live = (jnp.arange(OBS_DEV, dtype=jnp.int32)[None, :] < obs_count[:, None]).reshape(NOBS)
    live = live.astype(jnp.float32)

    def owner_block(items):
        block, values, alive = items
        wide = block.astype(jnp.float32)
        departure = jnp.einsum("olc,ol->oc", wide, values, precision=lax.Precision.HIGHEST)
        weighted = departure * error_inv[None, :]
        back = jnp.einsum("olc,oc->ol", wide, weighted, precision=lax.Precision.HIGHEST)
        return back * alive[:, None]

    adjoint_obs = lax.map(owner_block, (jacobian.reshape(PANELS, OBS_DEV, LEVELS, CH), columns.reshape(PANELS, OBS_DEV, LEVELS), live.reshape(PANELS, OBS_DEV)))
    adjoint_obs = adjoint_obs.reshape(NOBS, LEVELS)
    forcing = jnp.zeros((STEPS, LEVELS, PANELS * W * W), jnp.float32).at[earlier, :, obs_column].add(adjoint_obs)
    forcing = forcing.reshape(STEPS, LEVELS, PANELS, W, W)
    adjoint = forcing[STEPS - 1]
    for step in range(STEPS - 1, 0, -1):
        adjoint = adjoint_step(adjoint, coefs, center, vertical, side_pair, side_flip) + forcing[step - 1]
    adjoint = adjoint_step(adjoint, coefs, center, vertical, side_pair, side_flip)
    image = background_inv[:, None, None] * direction + adjoint.reshape(LEVELS, PANELS * W, W)
    norm_old = jnp.sum(residual * residual)
    alpha = norm_old / jnp.sum(direction * image)
    increment_new = increment + alpha * direction
    residual_new = residual - alpha * image
    norm_new = jnp.sum(residual_new * residual_new)
    direction_new = residual_new + (norm_new / norm_old) * direction
    return increment_new, residual_new, direction_new
```

```python
import jax
import jax.numpy as jnp
from jax import lax
from jax.experimental import pallas as pl
from jax.experimental.pallas import tpu as pltpu
import functools
from jax.sharding import PartitionSpec as P

STEPS = 4


def with_halo(block, sides, width):
    for axis, dim in sides:
        count = lax.axis_size(axis)
        forward = [(i, i + 1) for i in range(count - 1)]
        backward = [(target, source) for source, target in forward]
        low = lax.ppermute(
            lax.slice_in_dim(block, block.shape[dim] - width, None, axis=dim), axis, forward
        )
        high = lax.ppermute(lax.slice_in_dim(block, 0, width, axis=dim), axis, backward)
        block = jnp.concatenate([low, block, high], axis=dim)
    return block


def neighbours(strips, pair_rows, flip_rows):
    everyone = lax.all_gather(strips, ("tile", "sub"), axis=0, tiled=True)
    picked = everyone[pair_rows]
    return jnp.where(flip_rows[:, None, None] == 1, picked[:, :, ::-1], picked)


def level_padded(field):
    return with_halo(field, (("lev", 0),), 1)


def body(
    increment,
    residual,
    direction,
    wind_u,
    wind_v,
    diffusion,
    vertical,
    background_inv,
    side_pair,
    side_flip,
    obs_column,
    obs_time,
    obs_count,
    jacobian,
    error_inv,
):
    depth = increment.shape[0]
    width = increment.shape[2]
    slots = obs_column.shape[0]
    panels = lax.axis_size(("tile", "sub"))
    capacity = max(2, (2 * slots + panels - 1) // panels)
    panel = lax.axis_index(("tile", "sub"))
    first_level = lax.axis_index("lev") * depth
    mixing = lax.dynamic_slice_in_dim(diffusion, first_level, depth)[:, None, None]
    blending = lax.dynamic_slice_in_dim(vertical, first_level, depth)[:, None, None]
    prior = lax.dynamic_slice_in_dim(background_inv, first_level, depth)[:, None, None]
    pair_rows = lax.dynamic_index_in_dim(side_pair, panel, 0, keepdims=False)
    flip_rows = lax.dynamic_index_in_dim(side_flip, panel, 0, keepdims=False)
    speed_u = wind_u.astype(jnp.float32)
    speed_v = wind_v.astype(jnp.float32)
    coefs = (
        mixing + 0.5 * speed_u,
        mixing - 0.5 * speed_u,
        mixing + 0.5 * speed_v,
        mixing - 0.5 * speed_v,
    )
    center = 1.0 - 4.0 * mixing - 2.0 * blending

    def forward(field):
        strips = jnp.stack([field[:, 0, :], field[:, -1, :], field[:, :, 0], field[:, :, -1]])
        halos = neighbours(strips, pair_rows, flip_rows)
        north = jnp.concatenate([halos[0][:, None, :], field[:, :-1, :]], axis=1)
        south = jnp.concatenate([field[:, 1:, :], halos[1][:, None, :]], axis=1)
        west = jnp.concatenate([halos[2][:, :, None], field[:, :, :-1]], axis=2)
        east = jnp.concatenate([field[:, :, 1:], halos[3][:, :, None]], axis=2)
        padded = level_padded(field)
        return (
            center * field
            + coefs[0] * north
            + coefs[1] * south
            + coefs[2] * west
            + coefs[3] * east
            + blending * (padded[:-2] + padded[2:])
        )

    def adjoint(field):
        prods = [c * field for c in coefs]
        strips = jnp.stack(
            [prods[0][:, 0, :], prods[1][:, -1, :], prods[2][:, :, 0], prods[3][:, :, -1]]
        )
        halos = neighbours(strips, pair_rows, flip_rows)
        rows_term = jnp.concatenate([prods[0][:, 1:, :], halos[1][:, None, :]], axis=1)
        rows_term = rows_term + jnp.concatenate([halos[0][:, None, :], prods[1][:, :-1, :]], axis=1)
        cols_term = jnp.concatenate([prods[2][:, :, 1:], halos[3][:, :, None]], axis=2)
        cols_term = cols_term + jnp.concatenate([halos[2][:, :, None], prods[3][:, :, :-1]], axis=2)
        padded = level_padded(blending * field)
        return center * field + rows_term + cols_term + padded[:-2] + padded[2:]

    state = direction
    states = []
    for step in range(STEPS):
        state = forward(state)
        states.append(state.reshape(depth, width * width))
    history = jnp.stack(states, axis=0)
    area = width * width
    alive = jnp.arange(slots, dtype=jnp.int32) < obs_count[0]
    targets = obs_column // area
    cells = obs_column % area
    owned = (
        (targets[:, None] == jnp.arange(panels, dtype=jnp.int32)[None, :]) & alive[:, None]
    ).astype(jnp.int32)
    rank = jnp.sum((jnp.cumsum(owned, axis=0) - owned) * owned, axis=1)
    position = jnp.where(alive, targets * capacity + rank, panels * capacity)
    want_cell = (
        jnp.zeros((panels * capacity,), jnp.int32)
        .at[position]
        .set(cells, mode="drop")
        .reshape(panels, capacity)
    )
    want_time = (
        jnp.ones((panels * capacity,), jnp.int32)
        .at[position]
        .set(obs_time, mode="drop")
        .reshape(panels, capacity)
    )
    asked_cell = lax.all_to_all(want_cell, ("tile", "sub"), split_axis=0, concat_axis=0, tiled=True)
    asked_time = lax.all_to_all(want_time, ("tile", "sub"), split_axis=0, concat_axis=0, tiled=True)
    values = history[asked_time - 1, :, asked_cell]
    sent = lax.all_to_all(values, ("tile", "sub"), split_axis=0, concat_axis=0, tiled=True)
    gathered = sent.reshape(panels * capacity, depth)[jnp.minimum(position, panels * capacity - 1)]
    wide = jacobian.astype(jnp.float32)
    partial_value = jnp.einsum("olc,ol->oc", wide, gathered, precision=lax.Precision.HIGHEST)
    departure = lax.psum(partial_value, "lev")
    weighted = departure * error_inv[None, :]
    back = jnp.einsum("olc,oc->ol", wide, weighted, precision=lax.Precision.HIGHEST)
    back = back * alive.astype(jnp.float32)[:, None]
    outgoing = (
        jnp.zeros((panels * capacity, depth), jnp.float32)
        .at[position]
        .set(back, mode="drop")
        .reshape(panels, capacity, depth)
    )
    incoming = lax.all_to_all(outgoing, ("tile", "sub"), split_axis=0, concat_axis=0, tiled=True)
    flat_cell = asked_cell.reshape(panels * capacity)
    flat_time = asked_time.reshape(panels * capacity) - 1
    forcing = (
        jnp.zeros((STEPS, depth, area), jnp.float32)
        .at[flat_time, :, flat_cell]
        .add(incoming.reshape(panels * capacity, depth))
    )
    forcing = forcing.reshape(STEPS, depth, width, width)
    sensitivity = forcing[STEPS - 1]
    for step in range(STEPS - 1, 0, -1):
        sensitivity = adjoint(sensitivity) + forcing[step - 1]
    sensitivity = adjoint(sensitivity)
    image = prior * direction + sensitivity
    norm_old, curvature, cross, square = lax.psum(
        (
            jnp.sum(residual * residual),
            jnp.sum(direction * image),
            jnp.sum(residual * image),
            jnp.sum(image * image),
        ),
        ("tile", "lev", "sub"),
    )
    alpha = norm_old / curvature
    increment_new = increment + alpha * direction
    residual_new = residual - alpha * image
    norm_new = norm_old - 2.0 * alpha * cross + alpha * alpha * square
    direction_new = residual_new + norm_new / norm_old * direction
    return (increment_new, residual_new, direction_new)


MESH = pl.DeviceIdType.MESH
VM = pl.BlockSpec(memory_space=pltpu.VMEM)
SM = pl.BlockSpec(memory_space=pltpu.SMEM)
F32 = jnp.float32
NT = (((1,), (1,)), ((), ()))
TN = (((0,), (0,)), ((), ()))
NN = (((1,), (0,)), ((), ()))
OBS_ROWS = 8


def grid_sizes():
    return lax.axis_size("tile"), lax.axis_size("lev"), lax.axis_size("sub")


def place(flat, tiles, levs, subs):
    return {
        "tile": flat // (levs * subs),
        "lev": (flat // subs) % levs,
        "sub": flat % subs,
    }


def hail(peers):
    barrier = pltpu.get_barrier_semaphore()
    for peer in peers:
        pl.semaphore_signal(barrier, inc=1, device_id=peer, device_id_type=MESH)


def hailed(peers):
    pl.semaphore_wait(pltpu.get_barrier_semaphore(), len(peers))


def group_peers(sizes):
    tiles, levs, subs = sizes
    total = tiles * levs * subs
    me = (lax.axis_index("tile") * levs + lax.axis_index("lev")) * subs + lax.axis_index("sub")
    return [place(lax.rem(me + k, total), *sizes) for k in range(1, total)]


def halves(x):
    high = x.astype(jnp.bfloat16)
    return high, (x - high.astype(F32)).astype(jnp.bfloat16)


def dot2(values, onehot, dims):
    a, b = halves(values)
    return lax.dot_general(a, onehot, dims, preferred_element_type=F32) + lax.dot_general(
        b, onehot, dims, preferred_element_type=F32)


def dot2r(onehot, values, dims):
    a, b = halves(values)
    return lax.dot_general(onehot, a, dims, preferred_element_type=F32) + lax.dot_general(
        onehot, b, dims, preferred_element_type=F32)


def per_level(ref, levels, ndim):
    return jnp.stack([jnp.full((1,) * (ndim - 1), ref[l], F32) for l in range(levels)])


def edge_index(shape, rows, width):
    r = lax.broadcasted_iota(jnp.int32, shape, len(shape) - 2)
    return r if rows == width else jnp.where(r < rows // 2, r, r + (width - rows))


def column_of(halo, rows):
    width = halo.shape[-1]
    shape = (rows, width)
    hit = edge_index(shape, rows, width) == lax.broadcasted_iota(jnp.int32, shape, 1)
    return jnp.sum(jnp.where(hit, halo, 0.0), axis=-1, keepdims=True)


def shifted(x, axis, by, edge):
    n = x.shape[axis]
    rolled = pltpu.roll(x, by % n, axis)
    place_of = lax.broadcasted_iota(jnp.int32, x.shape[-2:], axis - (x.ndim - 2))
    return jnp.where(place_of == (0 if by == 1 else n - 1), edge, rolled)


def vertical_sum(x):
    levels = x.shape[0]
    parts = []
    for l in range(levels):
        total = jnp.zeros_like(x[l])
        if l > 0:
            total = total + x[l - 1]
        if l + 1 < levels:
            total = total + x[l + 1]
        parts.append(total)
    return jnp.stack(parts)


def forward_tile(x, c, center, vert, h):
    r, w = x.ndim - 2, x.ndim - 1
    rows = x.shape[r]
    return (
        center * x
        + c[0] * shifted(x, r, 1, h[0])
        + c[1] * shifted(x, r, -1, h[1])
        + c[2] * shifted(x, w, 1, column_of(h[2], rows))
        + c[3] * shifted(x, w, -1, column_of(h[3], rows))
        + vert * vertical_sum(x)
    )


def adjoint_tile(x, p, center, vert, h):
    r, w = x.ndim - 2, x.ndim - 1
    rows = x.shape[r]
    return (
        center * x
        + shifted(p[0], r, -1, h[1])
        + shifted(p[1], r, 1, h[0])
        + shifted(p[2], w, -1, column_of(h[3], rows))
        + shifted(p[3], w, 1, column_of(h[2], rows))
        + vertical_sum(vert * x)
    )


def swap(q):
    return (q[2], q[3], q[0], q[1])


def pairing_matrix(pair_ref, flip_ref, panels):
    sides = 4 * panels
    pair, turned = pair_ref[...].T, flip_ref[...].T
    code = (pair % 4) * panels + pair // 4 + sides * turned
    code = jnp.concatenate([code[:, k : k + 1] for k in range(4)], axis=0)
    return (code == lax.broadcasted_iota(jnp.int32, (sides, 2 * sides), 1)).astype(jnp.bfloat16)


def reversal(width):
    a = lax.broadcasted_iota(jnp.int32, (width, width), 0)
    b = lax.broadcasted_iota(jnp.int32, (width, width), 1)
    return (a + b == width - 1).astype(jnp.bfloat16)


def exchange(strips, choose, rev):
    levels, panels, _, width = strips[0].shape
    out = []
    for l in range(levels):
        s = jnp.concatenate([strips[k][l].reshape(panels, width) for k in range(4)], axis=0)
        both = jnp.concatenate([s, dot2(s, rev, NN)], axis=0)
        out.append(dot2r(choose, both, NN))
    h = jnp.stack(out)
    return [h[:, k * panels : (k + 1) * panels].reshape(levels, panels, 1, width) for k in range(4)]


def own_halos(h, store, panel):
    out = []
    for k in range(4):
        store[k] = h[k].reshape(store.shape[1:])
    for k in range(4):
        out.append(store[k, :, pl.ds(panel, 1), :])
    return out


def load_tiles(full, bands, dif_ref, ver_ref):
    levels, panels = bands.shape[0], bands.shape[1]
    tips = 2 * STEPS
    fields = {}
    m4, v4 = per_level(dif_ref, levels, 4), per_level(ver_ref, levels, 4)
    m3, v3 = per_level(dif_ref, levels, 3), per_level(ver_ref, levels, 3)

    def coefs(m, u, v):
        return (m + 0.5 * u, m - 0.5 * u, m + 0.5 * v, m - 0.5 * v)

    def band(f, which):
        start = (2 * f + which) * tips
        return bands[:, :, start : start + tips, :]

    ns = coefs(m4, band(1, 0), band(2, 0))
    we = swap(coefs(m4, band(1, 1), band(2, 1)))
    own = coefs(m3, full[:, 1], full[:, 2])
    scal4 = (1.0 - 4.0 * m4 - 2.0 * v4, v4)
    scal3 = (1.0 - 4.0 * m3 - 2.0 * v3, v3)
    return ns, we, own, scal4, scal3, band


def obs_rows(bands, width):
    base = 12 * STEPS
    column = bands[0, :, base, :].astype(jnp.int32)
    when = bands[0, :, base + 1, :].astype(jnp.int32)
    area = width * width
    live = column >= 0
    column = jnp.maximum(column, 0)
    panel = jnp.where(live, column // area, -1)
    cell = column % area
    return panel, cell // width, cell % width, when


def lanes_flat(x, slots):
    rows, width = x.shape
    per = width // slots
    lane = lax.broadcasted_iota(jnp.int32, (1, width), 1) // slots
    parts = []
    for q in range(0, rows, per):
        line = x[q : q + 1]
        for r in range(1, min(per, rows - q)):
            line = jnp.where(lane == r, pltpu.roll(x[q + r : q + r + 1], r * slots, 1), line)
        parts.append(line)
    return jnp.concatenate(parts, axis=1)


def whole_kernel(
    sizes, *refs,
):
    inputs, (img_out, alpha_out, beta_out), held = refs[:14], refs[14:17], refs[17:31]
    whole_steps(sizes, inputs, held, img_out, alpha_out, beta_out, *refs[31:])


def whole_steps(
    sizes, inputs, held, img_out, alpha_out, beta_out, landed,
    full, jall, bands, vall, gall, sall, store,
    fsend, frecv, zsend, zrecv, xsend, xrecv, csend, crecv, jsend, jrecv,
    gsend, grecv, vsend, vrecv, ssend, srecv,
):
    tiles, levs, subs = sizes
    tile, lev, sub = lax.axis_index("tile"), lax.axis_index("lev"), lax.axis_index("sub")
    loads = [
        pltpu.make_async_copy(src, dst, landed.at[k]) for k, (src, dst) in enumerate(zip(inputs, held))
    ]
    for load in loads[:3]:
        load.start()
    flat_peers = group_peers(sizes)
    hail(flat_peers)
    for load in loads[3:]:
        load.start()
    (dir_ref, wu_ref, wv_ref, col_ref, time_ref, count_ref, jac_ref, pair_ref, flip_ref, dif_ref,
     ver_ref, err_ref, inv_ref, res_ref) = held
    panels = tiles * subs
    everyone = panels * levs
    panel = tile * subs + sub
    me = (tile * levs + lev) * subs + sub
    slots = col_ref.shape[1]
    width = dir_ref.shape[2]
    tips = 2 * STEPS
    last = tips - 1
    for f, ref in enumerate((dir_ref, wu_ref, wv_ref)):
        loads[f].wait()
        x = ref[0].astype(F32)
        full[lev, f] = x
        xt = x.T
        rows = 2 * tips * f
        bands[lev, panel, rows : rows + STEPS] = x[:STEPS]
        bands[lev, panel, rows + STEPS : rows + tips] = x[width - STEPS :]
        bands[lev, panel, rows + tips : rows + tips + STEPS] = xt[:STEPS]
        bands[lev, panel, rows + tips + STEPS : rows + 2 * tips] = xt[width - STEPS :]
    base = 6 * tips
    for load in loads[3:6]:
        load.wait()
    alive = lax.broadcasted_iota(jnp.int32, (1, slots), 1) < count_ref[0]
    cols = jnp.where(alive, col_ref[...].astype(F32), -1.0)
    bands[lev, panel, base : base + OBS_ROWS] = jnp.full((OBS_ROWS, width), -1.0, F32)
    bands[lev, panel, base : base + 1, :slots] = cols
    bands[lev, panel, base + 1 : base + 2, :slots] = time_ref[...].astype(F32)
    loads[6].wait()
    jall[lev] = jac_ref[...].astype(F32)
    hailed(flat_peers)
    started = []

    def send(src, dst, ssem, rsem, where):
        copy = pltpu.make_async_remote_copy(
            src_ref=src, dst_ref=dst, send_sem=ssem, recv_sem=rsem,
            device_id=where, device_id_type=MESH)
        copy.start()
        started.append(copy)
        return copy

    def block(m, j):
        return bands.at[lax.rem(lev - m + levs, levs), lax.rem(tile - j + tiles, tiles) * subs + sub]

    arrivals_z, arrivals_x, arrivals_c, arrivals_f, arrivals_j = {}, {}, [], [], []

    def to_subs(m, j):
        for q in range(1, subs):
            arrivals_c.append(send(block(m, j), block(m, j), csend.at[q, m, j], crecv.at[q, m, j],
                                   {"sub": lax.rem(sub + q, subs)}))

    def to_levs(j):
        for m in range(1, levs):
            arrivals_x[m, j] = send(block(0, j), block(0, j), xsend.at[m, j], xrecv.at[m, j],
                                    {"lev": lax.rem(lev + m, levs)})

    for k in range(1, tiles):
        arrivals_z[k] = send(block(0, 0), block(0, 0), zsend.at[k], zrecv.at[k],
                             {"tile": lax.rem(tile + k, tiles)})
    to_levs(0)
    to_subs(0, 0)
    for m in range(1, levs):
        arrivals_f.append(send(full.at[lev], full.at[lev], fsend.at[m], frecv.at[m],
                               {"lev": lax.rem(lev + m, levs)}))
    order = sorted(range(1, tiles), key=lambda k: min(k, tiles - k))
    for k in order:
        arrivals_z[k].wait_recv()
        to_levs(k)
        to_subs(0, k)
    for m in range(1, levs):
        arrivals_j.append(send(jall.at[lev], jall.at[lev], jsend.at[m], jrecv.at[m],
                               {"lev": lax.rem(lev + m, levs)}))
    for load in loads[7:]:
        load.wait()
    choose = pairing_matrix(pair_ref, flip_ref, panels)
    rev = reversal(width)
    for j in [0] + order:
        for m in range(1, levs):
            arrivals_x[m, j].wait_recv()
            to_subs(m, j)
    for copy in arrivals_f + arrivals_c:
        copy.wait_recv()

    ns, we, own, scal4, scal3, band = load_tiles(full, bands, dif_ref, ver_ref)
    x_ns, x_we, x = band(0, 0), band(0, 1), full[:, 0]
    o_panel, o_i, o_j, o_t = obs_rows(bands, width)
    o_panel, o_i, o_j, o_t = [lanes_flat(v, slots) for v in (o_panel, o_i, o_j, o_t)]
    count = o_i.shape[1]
    spots = lax.broadcasted_iota(jnp.int32, (width, count), 0)
    is_i, is_j = spots == o_i, spots == o_j
    mine = is_i & (o_panel == panel)
    mine_i = mine.astype(jnp.bfloat16)
    values = [jnp.zeros(o_i.shape, F32) for _ in range(levs)]
    arrivals_g = []
    partners = []
    for k in range(1, panels):
        flat = lax.rem(panel + k, panels)
        partners.append((k, {"tile": flat // subs, "sub": lax.rem(flat, subs)}))
    for step in range(STEPS):
        strips = (x_ns[:, :, :1], x_ns[:, :, last:], x_we[:, :, :1], x_we[:, :, last:])
        h = exchange(strips, choose, rev)
        ho = own_halos(h, store, panel)
        x = forward_tile(x, own, *scal3, ho)
        if step + 1 < STEPS:
            x_ns, x_we = (
                forward_tile(x_ns, ns, *scal4, h),
                forward_tile(x_we, we, *scal4, swap(h)),
            )
        for l in range(levs):
            picked = dot2(x[l], mine_i, TN)
            got = jnp.sum(jnp.where(is_j, picked, 0.0), axis=0, keepdims=True)
            values[l] = jnp.where(o_t == step + 1, got, values[l])
        if step == STEPS - 2:
            for copy in arrivals_j:
                copy.wait_recv()
            e8 = jnp.broadcast_to(err_ref[...][None, :], (8, err_ref.shape[0]))
            row = 0
            gall[panel] = jnp.zeros(gall.shape[1:], F32)
            for a in range(levs):
                for b in range(a, levs):
                    g = lax.dot_general(
                        e8, jall[a] * jall[b], NT, precision=lax.Precision.HIGHEST,
                        preferred_element_type=F32)
                    gall[panel, row : row + 1, :slots] = g[:1]
                    row += 1
    lines = count // width
    for l in range(levs):
        for q in range(lines):
            vall[panel, l * lines + q : l * lines + q + 1] = values[l][:, q * width : (q + 1) * width]
    arrivals_v = [
        send(vall.at[panel], vall.at[panel], vsend.at[k], vrecv.at[k], where) for k, where in partners
    ]
    arrivals_g = [
        send(gall.at[panel], gall.at[panel], gsend.at[k], grecv.at[k], where) for k, where in partners
    ]
    at_i, at_j = is_i.astype(jnp.bfloat16), is_j.astype(jnp.bfloat16)
    edge = edge_index((tips, count), tips, width)
    on_i = jnp.concatenate([(edge == o_i) & (o_panel == p) for p in range(panels)], axis=0)
    on_j = jnp.concatenate([(edge == o_j) & (o_panel == p) for p in range(panels)], axis=0)
    for copy in arrivals_v + arrivals_g:
        copy.wait_recv()
    total = jnp.sum(vall[...], axis=0)
    columns = [
        jnp.concatenate([total[l * lines + q : l * lines + q + 1] for q in range(lines)], axis=1)
        for l in range(levs)
    ]
    gram = {}
    row = 0
    for a in range(levs):
        for b in range(a, levs):
            gram[a, b] = gram[b, a] = lanes_flat(gall[:, row, :], slots)
            row += 1
    back = []
    for a in range(levs):
        total = gram[a, 0] * columns[0]
        for b in range(1, levs):
            total = total + gram[a, b] * columns[b]
        back.append(jnp.where(o_panel >= 0, total, 0.0))

    def forcing(t):
        parts = [[], [], []]
        for l in range(levs):
            v = jnp.where(o_t == t, back[l], 0.0)
            parts[0].append(dot2(jnp.where(mine, v, 0.0), at_j, NT))
            parts[1].append(dot2(jnp.where(on_i, v, 0.0), at_j, NT).reshape(panels, tips, width))
            parts[2].append(dot2(jnp.where(on_j, v, 0.0), at_i, NT).reshape(panels, tips, width))
        return [jnp.stack(p) for p in parts]

    x, x_ns, x_we = forcing(STEPS)
    for step in range(STEPS - 1, -1, -1):
        p_ns = [c * x_ns for c in ns]
        p_we = [c * x_we for c in we]
        strips = (p_ns[0][:, :, :1], p_ns[1][:, :, last:], p_we[0][:, :, :1], p_we[1][:, :, last:])
        h = exchange(strips, choose, rev)
        ho = own_halos(h, store, panel)
        x = adjoint_tile(x, [c * x for c in own], *scal3, ho)
        if step > 0:
            f = forcing(step)
            x = x + f[0]
            x_ns = adjoint_tile(x_ns, p_ns, *scal4, h) + f[1]
            x_we = adjoint_tile(x_we, p_we, *scal4, swap(h)) + f[2]
    direction = dir_ref[0]
    image = jnp.zeros_like(direction)
    for l in range(levs):
        image = jnp.where(lev == l, x[l] + inv_ref[l] * direction, image)
    res = res_ref[0]
    pairs = ((res, res), (direction, image), (res, image), (image, image))
    sall[me] = jnp.concatenate(
        [jnp.sum(a * b, axis=0, keepdims=True) for a, b in pairs], axis=0)
    arrivals_s = [
        send(sall.at[me], sall.at[me], ssend.at[k], srecv.at[k], where)
        for k, where in enumerate(flat_peers)
    ]
    for copy in arrivals_s:
        copy.wait_recv()
    total = jnp.sum(jnp.sum(sall[...], axis=0), axis=1, keepdims=True)
    old, curvature, cross, square = [total[k : k + 1] for k in range(4)]
    alpha = old / curvature
    new = old - 2.0 * alpha * cross + alpha * alpha * square
    img_out[0] = image
    alpha_out[0] = jnp.broadcast_to(alpha, alpha_out.shape[1:])
    beta_out[0] = jnp.broadcast_to(new / old, beta_out.shape[1:])
    for copy in started:
        copy.wait_send()


def fused_body(
    increment, residual, direction, wind_u, wind_v, diffusion, vertical, background_inv,
    side_pair, side_flip, obs_column, obs_time, obs_count, jacobian, error_inv,
):
    sizes = grid_sizes()
    tiles, levs, subs = sizes
    panels = tiles * subs
    everyone = panels * levs
    width = increment.shape[2]
    slots, _, channels = jacobian.shape
    dma = pltpu.SemaphoreType.DMA
    band_rows = 12 * STEPS + OBS_ROWS
    per = width // slots
    lines = -(-panels // per)
    grams = levs * (levs + 1) // 2
    row = jax.ShapeDtypeStruct((1, 1, width), F32)
    inputs = (
        direction, wind_u, wind_v, obs_column[None, :], obs_time[None, :], obs_count,
        jacobian.reshape(slots, channels), side_pair.T, side_flip.T, diffusion, vertical,
        error_inv, background_inv, residual,
    )
    scalars = (5, 9, 10, 12)
    landing = [
        (pltpu.SMEM if k in scalars else pltpu.VMEM)(x.shape, x.dtype) for k, x in enumerate(inputs)
    ]
    image, alpha, beta = pl.pallas_call(
        functools.partial(whole_kernel, sizes),
        out_shape=(jax.ShapeDtypeStruct(increment.shape, F32), row, row),
        in_specs=[pl.BlockSpec(memory_space=pl.ANY)] * len(inputs),
        out_specs=(VM, VM, VM),
        scratch_shapes=landing + [
            dma((len(inputs),)),
            pltpu.VMEM((levs, 3, width, width), F32),
            pltpu.VMEM((levs, slots, channels), F32),
            pltpu.VMEM((levs, panels, band_rows, width), F32),
            pltpu.VMEM((panels, levs * lines, width), F32),
            pltpu.VMEM((panels, grams, width), F32),
            pltpu.VMEM((everyone, 4, width), F32),
            pltpu.VMEM((4, levs, panels, width), F32),
            dma((levs,)), dma((levs,)),
            dma((tiles,)), dma((tiles,)),
            dma((levs, tiles)), dma((levs, tiles)),
            dma((subs, levs, tiles)), dma((subs, levs, tiles)),
            dma((levs,)), dma((levs,)),
            dma((panels,)), dma((panels,)),
            dma((panels,)), dma((panels,)),
            dma((everyone,)), dma((everyone,)),
        ],
        compiler_params=pltpu.CompilerParams(
            collective_id=0, has_side_effects=True, vmem_limit_bytes=16 * 1024 * 1024),
        name="whole",
    )(*[x if x.size == 1 else pltpu.with_memory_space_constraint(x, pltpu.HBM) for x in inputs])
    left = residual - alpha * image
    return increment + alpha * direction, left, left + beta * direction


def chosen(*args):
    tiles, levs, subs = grid_sizes()
    increment, jacobian = args[0], args[13]
    width = increment.shape[2]
    gathered = tiles * subs * levs * (12 * STEPS + OBS_ROWS) * width * 4
    own = levs * (3 * width * width + jacobian.shape[0] * jacobian.shape[2]) * 4
    fits = (
        increment.shape[0] == 1
        and increment.shape[1] == width
        and width % jacobian.shape[0] == 0
        and (tiles * subs * jacobian.shape[0]) % width == 0
        and width >= 2 * STEPS
        and gathered <= 2 * own
    )
    return fused_body(*args) if fits else body(*args)


def solution(mesh):
    placed = (
        P(("member", "lev"), ("tile", "sub"), None),
        P(("member", "lev"), ("tile", "sub"), None),
        P(("member", "lev"), ("tile", "sub"), None),
        P(("member", "lev"), ("tile", "sub"), None),
        P(("member", "lev"), ("tile", "sub"), None),
        P(),
        P(),
        P(),
        P(),
        P(),
        P(("tile", "sub")),
        P(("tile", "sub")),
        P(("tile", "sub")),
        P(("tile", "sub"), "lev", None),
        P(),
    )
    return jax.shard_map(
        chosen,
        mesh=mesh,
        in_specs=placed,
        out_specs=(
            P(("member", "lev"), ("tile", "sub"), None),
            P(("member", "lev"), ("tile", "sub"), None),
            P(("member", "lev"), ("tile", "sub"), None),
        ),
        check_vma=False,
    )
```

```python
import jax
import jax.numpy as jnp
from jax import lax
from jax.experimental import pallas as pl
from jax.experimental.pallas import tpu as pltpu
import functools
from jax.sharding import PartitionSpec as P

STEPS = 4


def with_halo(block, sides, width):
    for axis, dim in sides:
        count = lax.axis_size(axis)
        forward = [(i, i + 1) for i in range(count - 1)]
        backward = [(target, source) for source, target in forward]
        low = lax.ppermute(
            lax.slice_in_dim(block, block.shape[dim] - width, None, axis=dim), axis, forward
        )
        high = lax.ppermute(lax.slice_in_dim(block, 0, width, axis=dim), axis, backward)
        block = jnp.concatenate([low, block, high], axis=dim)
    return block


def neighbours(strips, pair_rows, flip_rows):
    everyone = lax.all_gather(strips, ("tile", "sub"), axis=0, tiled=True)
    picked = everyone[pair_rows]
    return jnp.where(flip_rows[:, None, None] == 1, picked[:, :, ::-1], picked)


def level_padded(field):
    return with_halo(field, (("lev", 0),), 1)


def body(
    increment,
    residual,
    direction,
    wind_u,
    wind_v,
    diffusion,
    vertical,
    background_inv,
    side_pair,
    side_flip,
    obs_column,
    obs_time,
    obs_count,
    jacobian,
    error_inv,
):
    depth = increment.shape[0]
    width = increment.shape[2]
    slots = obs_column.shape[0]
    panels = lax.axis_size(("tile", "sub"))
    capacity = max(2, (2 * slots + panels - 1) // panels)
    panel = lax.axis_index(("tile", "sub"))
    first_level = lax.axis_index("lev") * depth
    mixing = lax.dynamic_slice_in_dim(diffusion, first_level, depth)[:, None, None]
    blending = lax.dynamic_slice_in_dim(vertical, first_level, depth)[:, None, None]
    prior = lax.dynamic_slice_in_dim(background_inv, first_level, depth)[:, None, None]
    pair_rows = lax.dynamic_index_in_dim(side_pair, panel, 0, keepdims=False)
    flip_rows = lax.dynamic_index_in_dim(side_flip, panel, 0, keepdims=False)
    speed_u = wind_u.astype(jnp.float32)
    speed_v = wind_v.astype(jnp.float32)
    coefs = (
        mixing + 0.5 * speed_u,
        mixing - 0.5 * speed_u,
        mixing + 0.5 * speed_v,
        mixing - 0.5 * speed_v,
    )
    center = 1.0 - 4.0 * mixing - 2.0 * blending

    def forward(field):
        strips = jnp.stack([field[:, 0, :], field[:, -1, :], field[:, :, 0], field[:, :, -1]])
        halos = neighbours(strips, pair_rows, flip_rows)
        north = jnp.concatenate([halos[0][:, None, :], field[:, :-1, :]], axis=1)
        south = jnp.concatenate([field[:, 1:, :], halos[1][:, None, :]], axis=1)
        west = jnp.concatenate([halos[2][:, :, None], field[:, :, :-1]], axis=2)
        east = jnp.concatenate([field[:, :, 1:], halos[3][:, :, None]], axis=2)
        padded = level_padded(field)
        return (
            center * field
            + coefs[0] * north
            + coefs[1] * south
            + coefs[2] * west
            + coefs[3] * east
            + blending * (padded[:-2] + padded[2:])
        )

    def adjoint(field):
        prods = [c * field for c in coefs]
        strips = jnp.stack(
            [prods[0][:, 0, :], prods[1][:, -1, :], prods[2][:, :, 0], prods[3][:, :, -1]]
        )
        halos = neighbours(strips, pair_rows, flip_rows)
        rows_term = jnp.concatenate([prods[0][:, 1:, :], halos[1][:, None, :]], axis=1)
        rows_term = rows_term + jnp.concatenate([halos[0][:, None, :], prods[1][:, :-1, :]], axis=1)
        cols_term = jnp.concatenate([prods[2][:, :, 1:], halos[3][:, :, None]], axis=2)
        cols_term = cols_term + jnp.concatenate([halos[2][:, :, None], prods[3][:, :, :-1]], axis=2)
        padded = level_padded(blending * field)
        return center * field + rows_term + cols_term + padded[:-2] + padded[2:]

    state = direction
    states = []
    for step in range(STEPS):
        state = forward(state)
        states.append(state.reshape(depth, width * width))
    history = jnp.stack(states, axis=0)
    area = width * width
    alive = jnp.arange(slots, dtype=jnp.int32) < obs_count[0]
    targets = obs_column // area
    cells = obs_column % area
    owned = (
        (targets[:, None] == jnp.arange(panels, dtype=jnp.int32)[None, :]) & alive[:, None]
    ).astype(jnp.int32)
    rank = jnp.sum((jnp.cumsum(owned, axis=0) - owned) * owned, axis=1)
    position = jnp.where(alive, targets * capacity + rank, panels * capacity)
    want_cell = (
        jnp.zeros((panels * capacity,), jnp.int32)
        .at[position]
        .set(cells, mode="drop")
        .reshape(panels, capacity)
    )
    want_time = (
        jnp.ones((panels * capacity,), jnp.int32)
        .at[position]
        .set(obs_time, mode="drop")
        .reshape(panels, capacity)
    )
    asked_cell = lax.all_to_all(want_cell, ("tile", "sub"), split_axis=0, concat_axis=0, tiled=True)
    asked_time = lax.all_to_all(want_time, ("tile", "sub"), split_axis=0, concat_axis=0, tiled=True)
    values = history[asked_time - 1, :, asked_cell]
    sent = lax.all_to_all(values, ("tile", "sub"), split_axis=0, concat_axis=0, tiled=True)
    gathered = sent.reshape(panels * capacity, depth)[jnp.minimum(position, panels * capacity - 1)]
    wide = jacobian.astype(jnp.float32)
    partial_value = jnp.einsum("olc,ol->oc", wide, gathered, precision=lax.Precision.HIGHEST)
    departure = lax.psum(partial_value, "lev")
    weighted = departure * error_inv[None, :]
    back = jnp.einsum("olc,oc->ol", wide, weighted, precision=lax.Precision.HIGHEST)
    back = back * alive.astype(jnp.float32)[:, None]
    outgoing = (
        jnp.zeros((panels * capacity, depth), jnp.float32)
        .at[position]
        .set(back, mode="drop")
        .reshape(panels, capacity, depth)
    )
    incoming = lax.all_to_all(outgoing, ("tile", "sub"), split_axis=0, concat_axis=0, tiled=True)
    flat_cell = asked_cell.reshape(panels * capacity)
    flat_time = asked_time.reshape(panels * capacity) - 1
    forcing = (
        jnp.zeros((STEPS, depth, area), jnp.float32)
        .at[flat_time, :, flat_cell]
        .add(incoming.reshape(panels * capacity, depth))
    )
    forcing = forcing.reshape(STEPS, depth, width, width)
    sensitivity = forcing[STEPS - 1]
    for step in range(STEPS - 1, 0, -1):
        sensitivity = adjoint(sensitivity) + forcing[step - 1]
    sensitivity = adjoint(sensitivity)
    image = prior * direction + sensitivity
    norm_old, curvature, cross, square = lax.psum(
        (
            jnp.sum(residual * residual),
            jnp.sum(direction * image),
            jnp.sum(residual * image),
            jnp.sum(image * image),
        ),
        ("tile", "lev", "sub"),
    )
    alpha = norm_old / curvature
    increment_new = increment + alpha * direction
    residual_new = residual - alpha * image
    norm_new = norm_old - 2.0 * alpha * cross + alpha * alpha * square
    direction_new = residual_new + norm_new / norm_old * direction
    return (increment_new, residual_new, direction_new)


MESH = pl.DeviceIdType.MESH
VM = pl.BlockSpec(memory_space=pltpu.VMEM)
F32 = jnp.float32
BF16 = jnp.bfloat16
NT = (((1,), (1,)), ((), ()))
TN = (((0,), (0,)), ((), ()))
NN = (((1,), (0,)), ((), ()))
FACTS = 3
MARGIN = 8
INPUTS = 14


def grid_sizes():
    return lax.axis_size("tile"), lax.axis_size("lev"), lax.axis_size("sub")


def slot_capacity(slots, panels):
    return max(2, (2 * slots + panels - 1) // panels)


def place(flat, tiles, levs, subs):
    return {
        "tile": flat // (levs * subs),
        "lev": (flat // subs) % levs,
        "sub": flat % subs,
    }


def hail(peers):
    barrier = pltpu.get_barrier_semaphore()
    for peer in peers:
        pl.semaphore_signal(barrier, inc=1, device_id=peer, device_id_type=MESH)


def hailed(peers):
    pl.semaphore_wait(pltpu.get_barrier_semaphore(), len(peers))


def group_peers(sizes):
    tiles, levs, subs = sizes
    total = tiles * levs * subs
    me = (lax.axis_index("tile") * levs + lax.axis_index("lev")) * subs + lax.axis_index("sub")
    return [place(lax.rem(me + k, total), *sizes) for k in range(1, total)]


def dot(a, b, dims, precision=None):
    return lax.dot_general(a, b, dims, precision=precision, preferred_element_type=F32)


def iota(shape, axis):
    return lax.broadcasted_iota(jnp.int32, shape, axis)


def fiota(shape, axis):
    return iota(shape, axis).astype(F32)


def halves(x):
    high = x.astype(BF16).astype(F32)
    return high, x - high


def per_level(ref, levels, ndim):
    return jnp.stack([jnp.full((1,) * (ndim - 1), ref[l], F32) for l in range(levels)])


def edge_index(shape, rows, width):
    r = iota(shape, len(shape) - 2)
    return jnp.where(r < rows // 2, r, r + (width - rows))


def column_of(halo, hit):
    return jnp.sum(jnp.where(hit, halo, 0.0), axis=-1, keepdims=True)


def shifted(x, axis, by, edge):
    n = x.shape[axis]
    rolled = pltpu.roll(x, by % n, axis)
    place_of = iota(x.shape[-2:], axis - (x.ndim - 2))
    return jnp.where(place_of == (0 if by == 1 else n - 1), edge, rolled)


def vertical_sum(x):
    levels = x.shape[0]
    parts = []
    for l in range(levels):
        total = jnp.zeros_like(x[l])
        if l > 0:
            total = total + x[l - 1]
        if l + 1 < levels:
            total = total + x[l + 1]
        parts.append(total)
    return jnp.stack(parts)


def forward_tile(x, c, center, vert, h, hit):
    r, w = x.ndim - 2, x.ndim - 1
    return (
        center * x
        + c[0] * shifted(x, r, 1, h[0])
        + c[1] * shifted(x, r, -1, h[1])
        + c[2] * shifted(x, w, 1, column_of(h[2], hit))
        + c[3] * shifted(x, w, -1, column_of(h[3], hit))
        + vert * vertical_sum(x)
    )


def adjoint_tile(x, p, center, vert, h, hit):
    r, w = x.ndim - 2, x.ndim - 1
    return (
        center * x
        + shifted(p[0], r, -1, h[1])
        + shifted(p[1], r, 1, h[0])
        + shifted(p[2], w, -1, column_of(h[3], hit))
        + shifted(p[3], w, 1, column_of(h[2], hit))
        + vertical_sum(vert * x)
    )


def swap(q):
    return (q[2], q[3], q[0], q[1])


def pairing_matrix(pair_ref, flip_ref, panels):
    sides = 4 * panels
    pair, turned = pair_ref[...].T, flip_ref[...].T
    code = (pair % 4) * panels + pair // 4 + sides * turned
    code = jnp.concatenate([code[:, k : k + 1] for k in range(4)], axis=0)
    shape = (sides, 2 * sides)
    picks = code == iota(shape, 1)
    return jnp.concatenate([picks.astype(F32)] * 2, axis=1).astype(BF16)


def reversal(width):
    shape = (2 * width, width)
    a = iota(shape, 0)
    a = jnp.where(a < width, a, a - width)
    return (a + iota(shape, 1) == width - 1).astype(BF16)


def exchange(strips, choose, rev):
    levels, panels, _, width = strips[0].shape
    sides = 4 * panels
    s = jnp.concatenate(
        [strips[k][l].reshape(panels, width) for l in range(levels) for k in range(4)], axis=0)
    high, low = halves(s)
    turned = dot(jnp.concatenate([high, low], axis=1).astype(BF16), rev, NN)
    thigh, tlow = halves(turned)
    both = jnp.concatenate(
        [
            jnp.concatenate([v[l * sides : (l + 1) * sides] for v in (high, thigh, low, tlow)], axis=0)
            for l in range(levels)
        ], axis=1)
    h = dot(choose, both.astype(BF16), NN)
    return [
        jnp.stack([
            h[k * panels : (k + 1) * panels, l * width : (l + 1) * width] for l in range(levels)
        ]).reshape(levels, panels, 1, width)
        for k in range(4)
    ]


def own_halos(h, store, panel):
    for k in range(4):
        store[k] = h[k].reshape(store.shape[1:])
    return [store[k, :, pl.ds(panel, 1), :] for k in range(4)]


def slot_rows(col, when, count, panels, area, width, capacity):
    slots = col.shape[1]
    alive = iota((1, slots), 1) < count
    panel = jnp.where(alive, col // area, -1)
    cell = col % area
    owned = (iota((panels, slots), 0) == panel).astype(F32)
    earlier = (iota((slots, slots), 0) < iota((slots, slots), 1)).astype(BF16)
    rank = jnp.sum(owned * dot(owned.astype(BF16), earlier, NN), axis=0, keepdims=True)
    slot = jnp.where(alive, panel.astype(F32) * capacity + rank, -1.0)
    spread = (fiota((panels * capacity, slots), 0) == slot).astype(BF16)
    facts = jnp.concatenate([cell // width + 1, cell % width + 1, when], axis=0).astype(F32)
    facts = jnp.concatenate([facts, jnp.zeros((8 - FACTS, slots), F32)], axis=0)
    return dot(facts.astype(BF16), spread, NT), spread


def by_panel(a, capacity):
    owners, width = a.shape
    mine = iota((owners, width), 1) // capacity == iota((owners, width), 0)
    slanted = pltpu.roll(a, 0, 1, stride=capacity, stride_axis=0)
    rows = []
    for p in range(width // capacity):
        r = pltpu.roll(slanted, width - p * capacity, 1) if p else slanted
        rows.append(jnp.sum(jnp.where(mine, r, 0.0), axis=0, keepdims=True))
    return jnp.concatenate(rows, axis=0)


def whole_kernel(sizes, capacity, *refs):
    tiles, levs, subs = sizes
    inputs, (img_out, alpha_out, beta_out) = refs[:INPUTS], refs[INPUTS : INPUTS + 3]
    held = refs[INPUTS + 3 : 2 * INPUTS + 3]
    (landed, stage, win, bands, jmine, jother, gall, vall, sall, rother, isent, igot, store, box,
     fsend, frecv, zsend, zrecv, xsend, xrecv, csend, crecv, jsend, jrecv, rsend, rrecv, isend, irecv,
     gsend, grecv, vsend, vrecv, ssend, srecv) = refs[2 * INPUTS + 3 :]
    (dir_ref, wu_ref, wv_ref, col_ref, time_ref, count_ref, jac_ref, err_ref, pair_ref, flip_ref,
     dif_ref, ver_ref, inv_ref, res_ref) = held
    loads = [
        pltpu.make_async_copy(src, dst, landed.at[k]) for k, (src, dst) in enumerate(zip(inputs, held))
    ]
    for load in loads[:6]:
        load.start()
    flat_peers = group_peers(sizes)
    hail(flat_peers)
    for load in loads[6:]:
        load.start()

    tile, lev, sub = lax.axis_index("tile"), lax.axis_index("lev"), lax.axis_index("sub")
    panels = tiles * subs
    panel = tile * subs + sub
    me = (tile * levs + lev) * subs + sub
    other = 1 - lev
    slots, channels = jac_ref.shape
    width = dir_ref.shape[2]
    area = width * width
    tips = 2 * STEPS
    last = tips - 1
    base = 6 * tips
    half = width // levs
    rows = half + MARGIN
    start = pl.multiple_of(lev * (width - rows), MARGIN)
    ostart = pl.multiple_of(other * (width - rows), MARGIN)
    mid = pl.multiple_of(lev * half, MARGIN)
    omid = pl.multiple_of(other * half, MARGIN)
    share = slots // levs

    for f, ref in enumerate((dir_ref, wu_ref, wv_ref)):
        loads[f].wait()
        x = ref[0].astype(F32)
        stage[f] = x
        xt = x.T
        at = 2 * tips * f
        bands[lev, panel, at : at + STEPS] = x[:STEPS]
        bands[lev, panel, at + STEPS : at + tips] = x[width - STEPS :]
        bands[lev, panel, at + tips : at + tips + STEPS] = xt[:STEPS]
        bands[lev, panel, at + tips + STEPS : at + 2 * tips] = xt[width - STEPS :]
    for load in loads[3:6]:
        load.wait()
    facts, spread = slot_rows(
        col_ref[...], time_ref[...], count_ref[0], panels, area, width, capacity)
    bands[lev, panel, base : base + FACTS] = facts[:FACTS]
    hailed(flat_peers)
    started = []

    def send(src, dst, ssem, rsem, where):
        copy = pltpu.make_async_remote_copy(
            src_ref=src, dst_ref=dst, send_sem=ssem, recv_sem=rsem,
            device_id=where, device_id_type=MESH)
        copy.start()
        started.append(copy)
        return copy

    def block(m, j):
        return bands.at[lax.rem(lev - m + levs, levs), lax.rem(tile - j + tiles, tiles) * subs + sub]

    arrivals_z, arrivals_x, arrivals_c = {}, {}, []
    across = {"lev": other}

    def to_subs(m, j):
        for q in range(1, subs):
            arrivals_c.append(send(block(m, j), block(m, j), csend.at[q, m, j], crecv.at[q, m, j],
                                   {"sub": lax.rem(sub + q, subs)}))

    def to_lev(j):
        arrivals_x[j] = send(block(0, j), block(0, j), xsend.at[j], xrecv.at[j], across)

    order = sorted(range(1, tiles), key=lambda k: min(k, tiles - k))
    for k in order:
        arrivals_z[k] = send(block(0, 0), block(0, 0), zsend.at[k], zrecv.at[k],
                             {"tile": lax.rem(tile + k, tiles)})
    to_lev(0)
    to_subs(0, 0)
    fields = send(stage.at[:, pl.ds(ostart, rows)], win.at[lev], fsend, frecv, across)
    for f in range(3):
        win[lev, f] = stage[f, pl.ds(start, rows)]
    for load in loads[6:]:
        load.wait()
    jmine[...] = jac_ref[...].astype(F32)
    choose = pairing_matrix(pair_ref, flip_ref, panels)
    rev = reversal(width)
    e8 = jnp.broadcast_to(err_ref[...][None, :], (8, channels))
    high = lax.Precision.HIGHEST

    def slotted(g):
        a, b = halves(g)
        both = jnp.concatenate([a, b], axis=0).astype(BF16)
        out = dot(both, spread, NT)
        return out[:1] + out[8:9]

    gall[lev, panel, 0:1] = slotted(dot(e8, jmine[...] * jmine[...], NT, high))
    for k in order:
        arrivals_z[k].wait_recv()
        to_lev(k)
        to_subs(0, k)
    jcopy = send(jmine.at[pl.ds(pl.multiple_of(other * share, MARGIN), share)], jother, jsend, jrecv, across)
    rcopy = send(res_ref.at[0, pl.ds(omid, half)], rother, rsend, rrecv, across)
    for j in [0] + order:
        arrivals_x[j].wait_recv()
        to_subs(1, j)
    for copy in [fields] + arrivals_c:
        copy.wait_recv()

    def band(f, which):
        at = (2 * f + which) * tips
        return bands[:, :, at : at + tips, :]

    def coefs(m, u, v):
        return (m + 0.5 * u, m - 0.5 * u, m + 0.5 * v, m - 0.5 * v)

    m4, v4 = per_level(dif_ref, levs, 4), per_level(ver_ref, levs, 4)
    m3, v3 = per_level(dif_ref, levs, 3), per_level(ver_ref, levs, 3)
    ns = coefs(m4, band(1, 0), band(2, 0))
    we = swap(coefs(m4, band(1, 1), band(2, 1)))
    own = coefs(m3, win[:, 1], win[:, 2])
    scal4 = (1.0 - 4.0 * m4 - 2.0 * v4, v4)
    scal3 = (1.0 - 4.0 * m3 - 2.0 * v3, v3)
    hit4 = edge_index((tips, width), tips, width) == iota((tips, width), 1)
    hit3 = iota((rows, width), 0) + start == iota((rows, width), 1)
    x_ns, x_we, x = band(0, 0), band(0, 1), win[:, 0]

    o_i, o_j, o_t = [by_panel(bands[0, :, base + k, :], capacity) for k in range(FACTS)]
    for k, v in enumerate((o_i, o_j, o_t)):
        box[k] = v
    s_i, s_j, s_t = [box[k, pl.ds(panel, 1), :] for k in range(FACTS)]
    line = iota((rows, width), 0)
    mine = (line + start + 1).astype(F32) == s_i
    inside = jnp.where((line >= lev * MARGIN) & (line < lev * MARGIN + half), 1.0, 0.0)
    here = jnp.where(mine, inside, 0.0)
    picked = [None] * levs
    for step in range(STEPS):
        strips = (x_ns[:, :, :1], x_ns[:, :, last:], x_we[:, :, :1], x_we[:, :, last:])
        h = exchange(strips, choose, rev)
        ho = own_halos(h, store.at[step % 2], panel)
        x = forward_tile(x, own, *scal3, ho, hit3)
        if step + 1 < STEPS:
            x_ns, x_we = (
                forward_tile(x_ns, ns, *scal4, h, hit4),
                forward_tile(x_we, we, *scal4, swap(h), hit4),
            )
        now = jnp.where(s_t == step + 1.0, here, 0.0)
        now = jnp.concatenate([now, now], axis=0).astype(BF16)
        for l in range(levs):
            got = dot(jnp.concatenate(halves(x[l]), axis=0).astype(BF16), now, TN)
            picked[l] = got if picked[l] is None else picked[l] + got
        if step == 1:
            jcopy.wait_recv()
            cross = dot(e8, jmine[pl.ds(pl.multiple_of(lev * share, MARGIN), share)] * jother[...], NT, high)
            cross = jnp.concatenate([cross] * levs, axis=1)
            cross = jnp.where(iota(cross.shape, 1) // share == lev, cross, 0.0)
            gall[lev, panel, 1:2] = slotted(cross)
            arrivals_g = [
                send(gall.at[lev, panel], gall.at[lev, panel], gsend.at[k], grecv.at[k], where)
                for k, where in enumerate(flat_peers)
            ]
    at_j = fiota((width, width), 0) + 1.0 == s_j
    for l in range(levs):
        vall[lev, panel, l : l + 1] = jnp.sum(jnp.where(at_j, picked[l], 0.0), axis=0, keepdims=True)
    arrivals_v = [
        send(vall.at[lev, panel], vall.at[lev, panel], vsend.at[k], vrecv.at[k], where)
        for k, where in enumerate(flat_peers)
    ]

    edge = edge_index((tips, width), tips, width).astype(F32) + 1.0
    spots = fiota((width, width), 0) + 1.0

    def onehots(p, a, b):
        tip = jnp.concatenate(
            [jnp.where((edge == a[p : p + 1]) & (o_t[p : p + 1] == t), 1.0, 0.0)
             for t in range(1, STEPS + 1)], axis=0)
        along = jnp.where(spots == b[p : p + 1], 1.0, 0.0)
        return tip, jnp.concatenate([along, along], axis=1).astype(BF16)

    hot_ns = [onehots(p, o_i, o_j) for p in range(panels)]
    hot_we = [onehots(p, o_j, o_i) for p in range(panels)]
    rows_own = jnp.concatenate(
        [jnp.where(mine & (s_t == t), 1.0, 0.0) for t in range(1, STEPS + 1)], axis=0)
    rows_own = jnp.concatenate([rows_own, rows_own], axis=1).astype(BF16)
    for copy in arrivals_g:
        copy.wait_recv()
    gram = {(l, l): by_panel(gall[l, :, 0, :], capacity) for l in range(levs)}
    gram[0, 1] = gram[1, 0] = by_panel(gall[0, :, 1, :] + gall[1, :, 1, :], capacity)
    for copy in arrivals_v:
        copy.wait_recv()
    total = vall[0] + vall[1]
    back = [gram[a, 0] * total[:, 0] + gram[a, 1] * total[:, 1] for a in range(levs)]
    parts = [halves(b) for b in back]

    def band_forcing(hot):
        out = []
        for p in range(panels):
            tip, along = hot[p]
            left = jnp.concatenate(
                [jnp.concatenate([tip * v[p : p + 1] for v in parts[l]], axis=1) for l in range(levs)],
                axis=0)
            out.append(dot(left.astype(BF16), along, NT))
        return [
            jnp.stack([
                jnp.stack([o[(l * STEPS + t) * tips : (l * STEPS + t + 1) * tips] for o in out])
                for l in range(levs)])
            for t in range(STEPS)
        ]

    for l in range(levs):
        box[l] = back[l]
    scaled = []
    for l in range(levs):
        v = halves(box[l, pl.ds(panel, 1), :])
        scaled.append(jnp.concatenate([jnp.where(at_j, w, 0.0) for w in v], axis=1))
    flat = dot(rows_own, jnp.concatenate(scaled, axis=0).astype(BF16), NT)
    force = [
        jnp.stack([flat[t * rows : (t + 1) * rows, l * width : (l + 1) * width] for l in range(levs)])
        for t in range(STEPS)
    ]
    force_ns, force_we = band_forcing(hot_ns), band_forcing(hot_we)
    x, x_ns, x_we = force[-1], force_ns[-1], force_we[-1]
    for step in range(STEPS - 1, -1, -1):
        p_ns = [c * x_ns for c in ns]
        p_we = [c * x_we for c in we]
        strips = (p_ns[0][:, :, :1], p_ns[1][:, :, last:], p_we[0][:, :, :1], p_we[1][:, :, last:])
        h = exchange(strips, choose, rev)
        ho = own_halos(h, store.at[step % 2], panel)
        x = adjoint_tile(x, [c * x for c in own], *scal3, ho, hit3)
        if step > 0:
            x = x + force[step - 1]
            x_ns = adjoint_tile(x_ns, p_ns, *scal4, h, hit4) + force_ns[step - 1]
            x_we = adjoint_tile(x_we, p_we, *scal4, swap(h), hit4) + force_we[step - 1]

    rcopy.wait_recv()
    x = jnp.where(lev == 0, x[:, :half], x[:, rows - half :])
    direction = [win[l, 0, pl.ds(pl.multiple_of(lev * MARGIN, MARGIN), half)] for l in range(levs)]
    image = [x[l] + inv_ref[l] * direction[l] for l in range(levs)]
    own_res, other_res = res_ref[0, pl.ds(mid, half)], rother[...]
    sums = None
    for l in range(levs):
        res = jnp.where(lev == l, own_res, other_res)
        pairs = ((res, res), (direction[l], image[l]), (res, image[l]), (image[l], image[l]))
        part = jnp.concatenate([jnp.sum(a * b, axis=0, keepdims=True) for a, b in pairs], axis=0)
        sums = part if sums is None else sums + part
    sall[me] = sums
    arrivals_s = [
        send(sall.at[me], sall.at[me], ssend.at[k], srecv.at[k], where)
        for k, where in enumerate(flat_peers)
    ]
    isent[...] = jnp.where(lev == 0, image[1], image[0])
    icopy = send(isent, igot, isend, irecv, across)
    img_out[0, pl.ds(mid, half)] = jnp.where(lev == 0, image[0], image[1])
    icopy.wait_recv()
    img_out[0, pl.ds(omid, half)] = igot[...]
    for copy in arrivals_s:
        copy.wait_recv()
    total = jnp.sum(jnp.sum(sall[...], axis=0), axis=1, keepdims=True)
    old, curvature, cross, square = [total[k : k + 1] for k in range(4)]
    alpha = old / curvature
    new = old - 2.0 * alpha * cross + alpha * alpha * square
    alpha_out[0] = jnp.broadcast_to(alpha, alpha_out.shape[1:])
    beta_out[0] = jnp.broadcast_to(new / old, beta_out.shape[1:])
    for copy in started:
        copy.wait_send()


def fused_body(
    increment, residual, direction, wind_u, wind_v, diffusion, vertical, background_inv,
    side_pair, side_flip, obs_column, obs_time, obs_count, jacobian, error_inv,
):
    sizes = grid_sizes()
    tiles, levs, subs = sizes
    panels = tiles * subs
    everyone = panels * levs
    width = increment.shape[2]
    slots, _, channels = jacobian.shape
    half = width // levs
    rows = half + MARGIN
    dma = pltpu.SemaphoreType.DMA
    inputs = (
        direction, wind_u, wind_v, obs_column[None, :], obs_time[None, :], obs_count,
        jacobian.reshape(slots, channels), error_inv, side_pair.T, side_flip.T, diffusion, vertical,
        background_inv, residual,
    )
    scalars = (5, 10, 11, 12)
    landing = [
        (pltpu.SMEM if k in scalars else pltpu.VMEM)(x.shape, x.dtype) for k, x in enumerate(inputs)
    ]
    row = jax.ShapeDtypeStruct((1, 1, width), F32)
    image, alpha, beta = pl.pallas_call(
        functools.partial(whole_kernel, sizes, slot_capacity(slots, panels)),
        out_shape=(jax.ShapeDtypeStruct(increment.shape, F32), row, row),
        in_specs=[pl.BlockSpec(memory_space=pl.ANY)] * len(inputs),
        out_specs=(VM, VM, VM),
        scratch_shapes=landing + [
            dma((len(inputs),)),
            pltpu.VMEM((3, width, width), F32),
            pltpu.VMEM((levs, 3, rows, width), F32),
            pltpu.VMEM((levs, panels, 12 * STEPS + FACTS, width), F32),
            pltpu.VMEM((slots, channels), F32),
            pltpu.VMEM((slots // levs, channels), F32),
            pltpu.VMEM((levs, panels, 2, width), F32),
            pltpu.VMEM((levs, panels, levs, width), F32),
            pltpu.VMEM((everyone, 4, width), F32),
            pltpu.VMEM((half, width), F32),
            pltpu.VMEM((half, width), F32),
            pltpu.VMEM((half, width), F32),
            pltpu.VMEM((2, 4, levs, panels, width), F32),
            pltpu.VMEM((FACTS, panels, width), F32),
            dma, dma,
            dma((tiles,)), dma((tiles,)),
            dma((tiles,)), dma((tiles,)),
            dma((subs, levs, tiles)), dma((subs, levs, tiles)),
            dma, dma,
            dma, dma,
            dma, dma,
            dma((everyone,)), dma((everyone,)),
            dma((everyone,)), dma((everyone,)),
            dma((everyone,)), dma((everyone,)),
        ],
        compiler_params=pltpu.CompilerParams(
            collective_id=0, has_side_effects=True, vmem_limit_bytes=16 * 1024 * 1024),
        name="whole",
    )(*[x if x.size == 1 else pltpu.with_memory_space_constraint(x, pltpu.HBM) for x in inputs])
    left = residual - alpha * image
    return increment + alpha * direction, left, left + beta * direction


def chosen(*args):
    tiles, levs, subs = grid_sizes()
    increment, jacobian = args[0], args[13]
    width, slots, panels = increment.shape[2], jacobian.shape[0], tiles * subs
    fits = (
        levs == 2
        and increment.shape[0] == 1
        and increment.shape[1] == width
        and panels * slot_capacity(slots, panels) == width
        and panels == 8
        and slots % (8 * levs) == 0
        and width % (8 * levs) == 0
        and STEPS <= MARGIN
        and width >= 2 * STEPS
    )
    return fused_body(*args) if fits else body(*args)


def solution(mesh):
    placed = (
        P(("member", "lev"), ("tile", "sub"), None),
        P(("member", "lev"), ("tile", "sub"), None),
        P(("member", "lev"), ("tile", "sub"), None),
        P(("member", "lev"), ("tile", "sub"), None),
        P(("member", "lev"), ("tile", "sub"), None),
        P(),
        P(),
        P(),
        P(),
        P(),
        P(("tile", "sub")),
        P(("tile", "sub")),
        P(("tile", "sub")),
        P(("tile", "sub"), "lev", None),
        P(),
    )
    return jax.shard_map(
        chosen,
        mesh=mesh,
        in_specs=placed,
        out_specs=(
            P(("member", "lev"), ("tile", "sub"), None),
            P(("member", "lev"), ("tile", "sub"), None),
            P(("member", "lev"), ("tile", "sub"), None),
        ),
        check_vma=False,
    )
```

```python
import jax
import jax.numpy as jnp
from jax import lax
from jax.experimental import pallas as pl
from jax.experimental.pallas import tpu as pltpu
import functools
from jax.sharding import PartitionSpec as P

STEPS = 4


def with_halo(block, sides, width):
    for axis, dim in sides:
        count = lax.axis_size(axis)
        forward = [(i, i + 1) for i in range(count - 1)]
        backward = [(target, source) for source, target in forward]
        low = lax.ppermute(
            lax.slice_in_dim(block, block.shape[dim] - width, None, axis=dim), axis, forward
        )
        high = lax.ppermute(lax.slice_in_dim(block, 0, width, axis=dim), axis, backward)
        block = jnp.concatenate([low, block, high], axis=dim)
    return block


def neighbours(strips, pair_rows, flip_rows):
    everyone = lax.all_gather(strips, ("tile", "sub"), axis=0, tiled=True)
    picked = everyone[pair_rows]
    return jnp.where(flip_rows[:, None, None] == 1, picked[:, :, ::-1], picked)


def level_padded(field):
    return with_halo(field, (("lev", 0),), 1)


def body(
    increment,
    residual,
    direction,
    wind_u,
    wind_v,
    diffusion,
    vertical,
    background_inv,
    side_pair,
    side_flip,
    obs_column,
    obs_time,
    obs_count,
    jacobian,
    error_inv,
):
    depth = increment.shape[0]
    width = increment.shape[2]
    slots = obs_column.shape[0]
    panels = lax.axis_size(("tile", "sub"))
    capacity = max(2, (2 * slots + panels - 1) // panels)
    panel = lax.axis_index(("tile", "sub"))
    first_level = lax.axis_index("lev") * depth
    mixing = lax.dynamic_slice_in_dim(diffusion, first_level, depth)[:, None, None]
    blending = lax.dynamic_slice_in_dim(vertical, first_level, depth)[:, None, None]
    prior = lax.dynamic_slice_in_dim(background_inv, first_level, depth)[:, None, None]
    pair_rows = lax.dynamic_index_in_dim(side_pair, panel, 0, keepdims=False)
    flip_rows = lax.dynamic_index_in_dim(side_flip, panel, 0, keepdims=False)
    speed_u = wind_u.astype(jnp.float32)
    speed_v = wind_v.astype(jnp.float32)
    coefs = (
        mixing + 0.5 * speed_u,
        mixing - 0.5 * speed_u,
        mixing + 0.5 * speed_v,
        mixing - 0.5 * speed_v,
    )
    center = 1.0 - 4.0 * mixing - 2.0 * blending

    def forward(field):
        strips = jnp.stack([field[:, 0, :], field[:, -1, :], field[:, :, 0], field[:, :, -1]])
        halos = neighbours(strips, pair_rows, flip_rows)
        north = jnp.concatenate([halos[0][:, None, :], field[:, :-1, :]], axis=1)
        south = jnp.concatenate([field[:, 1:, :], halos[1][:, None, :]], axis=1)
        west = jnp.concatenate([halos[2][:, :, None], field[:, :, :-1]], axis=2)
        east = jnp.concatenate([field[:, :, 1:], halos[3][:, :, None]], axis=2)
        padded = level_padded(field)
        return (
            center * field
            + coefs[0] * north
            + coefs[1] * south
            + coefs[2] * west
            + coefs[3] * east
            + blending * (padded[:-2] + padded[2:])
        )

    def adjoint(field):
        prods = [c * field for c in coefs]
        strips = jnp.stack(
            [prods[0][:, 0, :], prods[1][:, -1, :], prods[2][:, :, 0], prods[3][:, :, -1]]
        )
        halos = neighbours(strips, pair_rows, flip_rows)
        rows_term = jnp.concatenate([prods[0][:, 1:, :], halos[1][:, None, :]], axis=1)
        rows_term = rows_term + jnp.concatenate([halos[0][:, None, :], prods[1][:, :-1, :]], axis=1)
        cols_term = jnp.concatenate([prods[2][:, :, 1:], halos[3][:, :, None]], axis=2)
        cols_term = cols_term + jnp.concatenate([halos[2][:, :, None], prods[3][:, :, :-1]], axis=2)
        padded = level_padded(blending * field)
        return center * field + rows_term + cols_term + padded[:-2] + padded[2:]

    state = direction
    states = []
    for step in range(STEPS):
        state = forward(state)
        states.append(state.reshape(depth, width * width))
    history = jnp.stack(states, axis=0)
    area = width * width
    alive = jnp.arange(slots, dtype=jnp.int32) < obs_count[0]
    targets = obs_column // area
    cells = obs_column % area
    owned = (
        (targets[:, None] == jnp.arange(panels, dtype=jnp.int32)[None, :]) & alive[:, None]
    ).astype(jnp.int32)
    rank = jnp.sum((jnp.cumsum(owned, axis=0) - owned) * owned, axis=1)
    position = jnp.where(alive, targets * capacity + rank, panels * capacity)
    want_cell = (
        jnp.zeros((panels * capacity,), jnp.int32)
        .at[position]
        .set(cells, mode="drop")
        .reshape(panels, capacity)
    )
    want_time = (
        jnp.ones((panels * capacity,), jnp.int32)
        .at[position]
        .set(obs_time, mode="drop")
        .reshape(panels, capacity)
    )
    asked_cell = lax.all_to_all(want_cell, ("tile", "sub"), split_axis=0, concat_axis=0, tiled=True)
    asked_time = lax.all_to_all(want_time, ("tile", "sub"), split_axis=0, concat_axis=0, tiled=True)
    values = history[asked_time - 1, :, asked_cell]
    sent = lax.all_to_all(values, ("tile", "sub"), split_axis=0, concat_axis=0, tiled=True)
    gathered = sent.reshape(panels * capacity, depth)[jnp.minimum(position, panels * capacity - 1)]
    wide = jacobian.astype(jnp.float32)
    partial_value = jnp.einsum("olc,ol->oc", wide, gathered, precision=lax.Precision.HIGHEST)
    departure = lax.psum(partial_value, "lev")
    weighted = departure * error_inv[None, :]
    back = jnp.einsum("olc,oc->ol", wide, weighted, precision=lax.Precision.HIGHEST)
    back = back * alive.astype(jnp.float32)[:, None]
    outgoing = (
        jnp.zeros((panels * capacity, depth), jnp.float32)
        .at[position]
        .set(back, mode="drop")
        .reshape(panels, capacity, depth)
    )
    incoming = lax.all_to_all(outgoing, ("tile", "sub"), split_axis=0, concat_axis=0, tiled=True)
    flat_cell = asked_cell.reshape(panels * capacity)
    flat_time = asked_time.reshape(panels * capacity) - 1
    forcing = (
        jnp.zeros((STEPS, depth, area), jnp.float32)
        .at[flat_time, :, flat_cell]
        .add(incoming.reshape(panels * capacity, depth))
    )
    forcing = forcing.reshape(STEPS, depth, width, width)
    sensitivity = forcing[STEPS - 1]
    for step in range(STEPS - 1, 0, -1):
        sensitivity = adjoint(sensitivity) + forcing[step - 1]
    sensitivity = adjoint(sensitivity)
    image = prior * direction + sensitivity
    norm_old, curvature, cross, square = lax.psum(
        (
            jnp.sum(residual * residual),
            jnp.sum(direction * image),
            jnp.sum(residual * image),
            jnp.sum(image * image),
        ),
        ("tile", "lev", "sub"),
    )
    alpha = norm_old / curvature
    increment_new = increment + alpha * direction
    residual_new = residual - alpha * image
    norm_new = norm_old - 2.0 * alpha * cross + alpha * alpha * square
    direction_new = residual_new + norm_new / norm_old * direction
    return (increment_new, residual_new, direction_new)


MESH = pl.DeviceIdType.MESH
VM = pl.BlockSpec(memory_space=pltpu.VMEM)
F32 = jnp.float32
BF16 = jnp.bfloat16
NT = (((1,), (1,)), ((), ()))
TN = (((0,), (0,)), ((), ()))
NN = (((1,), (0,)), ((), ()))
FACTS = 3
MARGIN = 8
INPUTS = 14


def grid_sizes():
    return lax.axis_size("tile"), lax.axis_size("lev"), lax.axis_size("sub")


def slot_capacity(slots, panels):
    return max(2, (2 * slots + panels - 1) // panels)


def hail(peers):
    barrier = pltpu.get_barrier_semaphore()
    for peer in peers:
        pl.semaphore_signal(barrier, inc=1, device_id=peer, device_id_type=MESH)


def hailed(peers):
    pl.semaphore_wait(pltpu.get_barrier_semaphore(), len(peers))


def group_peers(sizes):
    axes = ("tile", "lev", "sub")
    steps = [(t, l, u) for t in range(sizes[0]) for l in range(sizes[1]) for u in range(sizes[2])]
    steps.sort(key=lambda d: (-min(d[0], sizes[0] - d[0]), -d[1], -d[2]))
    return [
        {axis: lax.rem(lax.axis_index(axis) + by, size) for axis, by, size in zip(axes, d, sizes)}
        for d in steps if any(d)
    ]


def by_distance(tile, tiles):
    table = [sorted((t for t in range(tiles) if t != me), key=lambda t: abs(t - me)) for me in range(tiles)]
    picks = []
    for k in range(tiles - 1):
        pick = jnp.int32(table[0][k])
        for me in range(1, tiles):
            pick = jnp.where(tile == me, table[me][k], pick)
        picks.append(pick)
    return picks


def dot(a, b, dims, precision=None):
    return lax.dot_general(a, b, dims, precision=precision, preferred_element_type=F32)


def iota(shape, axis):
    return lax.broadcasted_iota(jnp.int32, shape, axis)


def fiota(shape, axis):
    return iota(shape, axis).astype(F32)


def halves(x):
    high = x.astype(BF16).astype(F32)
    return high, x - high


def per_level(ref, levels, ndim):
    return jnp.stack([jnp.full((1,) * (ndim - 1), ref[l], F32) for l in range(levels)])


def edge_index(shape, rows, width):
    r = iota(shape, len(shape) - 2)
    return jnp.where(r < rows // 2, r, r + (width - rows))


def column_of(halo, hit):
    return jnp.sum(jnp.where(hit, halo, 0.0), axis=-1, keepdims=True)


def shifted(x, axis, by, edge):
    n = x.shape[axis]
    rolled = pltpu.roll(x, by % n, axis)
    place_of = iota(x.shape[-2:], axis - (x.ndim - 2))
    return jnp.where(place_of == (0 if by == 1 else n - 1), edge, rolled)


def vertical_sum(x):
    levels = x.shape[0]
    parts = []
    for l in range(levels):
        total = jnp.zeros_like(x[l])
        if l > 0:
            total = total + x[l - 1]
        if l + 1 < levels:
            total = total + x[l + 1]
        parts.append(total)
    return jnp.stack(parts)


def forward_tile(x, c, center, vert, h, hit):
    r, w = x.ndim - 2, x.ndim - 1
    return (
        center * x
        + c[0] * shifted(x, r, 1, h[0])
        + c[1] * shifted(x, r, -1, h[1])
        + c[2] * shifted(x, w, 1, column_of(h[2], hit))
        + c[3] * shifted(x, w, -1, column_of(h[3], hit))
        + vert * vertical_sum(x)
    )


def adjoint_tile(x, p, center, vert, h, hit):
    r, w = x.ndim - 2, x.ndim - 1
    return (
        center * x
        + shifted(p[0], r, -1, h[1])
        + shifted(p[1], r, 1, h[0])
        + shifted(p[2], w, -1, column_of(h[3], hit))
        + shifted(p[3], w, 1, column_of(h[2], hit))
        + vertical_sum(vert * x)
    )


def swap(q):
    return (q[2], q[3], q[0], q[1])


def turned(x):
    width = x.shape[1]
    back = width - 1 - iota((8, width), 1)
    return jnp.concatenate(
        [jnp.take_along_axis(x[r : r + 8], back, axis=1) for r in range(0, x.shape[0], 8)], axis=0)


def partner_rows(pair_ref, flip_ref, levels, panels):
    sides = 4 * panels

    def row(k, p):
        pair = pair_ref[k, p]
        return (flip_ref[k, p] * levels * sides) + (pair % 4) * panels + pair // 4

    return row


def exchange(strips, store, row, panel):
    levels, panels, _, width = strips[0].shape
    sides = 4 * panels
    s = jnp.concatenate(
        [strips[k][l].reshape(panels, width) for l in range(levels) for k in range(4)], axis=0)
    store[: levels * sides] = s
    store[levels * sides :] = turned(s)

    def strip(k, p, l):
        return store[pl.ds(row(k, p) + l * sides, 1), :]

    every = [
        jnp.stack([jnp.stack([strip(k, p, l) for p in range(panels)]) for l in range(levels)])
        for k in range(4)
    ]
    return every, [jnp.stack([strip(k, panel, l) for l in range(levels)]) for k in range(4)]


def slot_rows(col, when, count, panels, area, width, capacity):
    slots = col.shape[1]
    alive = iota((1, slots), 1) < count
    panel = jnp.where(alive, col // area, -1)
    cell = col % area
    owned = (iota((panels, slots), 0) == panel).astype(F32)
    earlier = (iota((slots, slots), 0) < iota((slots, slots), 1)).astype(BF16)
    rank = jnp.sum(owned * dot(owned.astype(BF16), earlier, NN), axis=0, keepdims=True)
    slot = jnp.where(alive, panel.astype(F32) * capacity + rank, -1.0)
    spread = (fiota((panels * capacity, slots), 0) == slot).astype(BF16)
    facts = jnp.concatenate([cell // width + 1, cell % width + 1, when], axis=0).astype(F32)
    facts = jnp.concatenate([facts, jnp.zeros((8 - FACTS, slots), F32)], axis=0)
    return dot(facts.astype(BF16), spread, NT), spread


def by_panel(a, capacity):
    owners, width = a.shape
    mine = iota((owners, width), 1) // capacity == iota((owners, width), 0)
    slanted = pltpu.roll(a, 0, 1, stride=capacity, stride_axis=0)
    rows = []
    for p in range(width // capacity):
        r = pltpu.roll(slanted, width - p * capacity, 1) if p else slanted
        rows.append(jnp.sum(jnp.where(mine, r, 0.0), axis=0, keepdims=True))
    return jnp.concatenate(rows, axis=0)


def whole_kernel(sizes, capacity, *refs):
    tiles, levs, subs = sizes
    inputs, (img_out, alpha_out, beta_out) = refs[:INPUTS], refs[INPUTS : INPUTS + 3]
    held = refs[INPUTS + 3 : 2 * INPUTS + 3]
    (landed, stage, win, bands, jmine, jother, gall, vall, sall, rother, isent, igot, store, box,
     fsend, frecv, zsend, zrecv, xsend, xrecv, csend, crecv, jsend, jrecv, rsend, rrecv, isend, irecv,
     gsend, grecv, vsend, vrecv, ssend, srecv) = refs[2 * INPUTS + 3 :]
    (dir_ref, wu_ref, wv_ref, col_ref, time_ref, count_ref, jac_ref, err_ref, pair_ref, flip_ref,
     dif_ref, ver_ref, inv_ref, res_ref) = held
    loads = [
        pltpu.make_async_copy(src, dst, landed.at[k]) for k, (src, dst) in enumerate(zip(inputs, held))
    ]
    flat_peers = group_peers(sizes)
    near = [{axis: lax.rem(lax.axis_index(axis) + k, size)}
            for axis, size in zip(("tile", "lev", "sub"), sizes) for k in range(1, size)]
    hail(near)
    for load in loads[:6]:
        load.start()
    for load in loads[6:]:
        load.start()

    tile, lev, sub = lax.axis_index("tile"), lax.axis_index("lev"), lax.axis_index("sub")
    panels = tiles * subs
    panel = tile * subs + sub
    me = (tile * levs + lev) * subs + sub
    other = 1 - lev
    slots, channels = jac_ref.shape
    width = dir_ref.shape[2]
    area = width * width
    tips = 2 * STEPS
    last = tips - 1
    base = 6 * tips
    half = width // levs
    rows = half + MARGIN
    start = pl.multiple_of(lev * (width - rows), MARGIN)
    ostart = pl.multiple_of(other * (width - rows), MARGIN)
    mid = pl.multiple_of(lev * half, MARGIN)
    omid = pl.multiple_of(other * half, MARGIN)
    share = slots // levs

    for f, ref in enumerate((dir_ref, wu_ref, wv_ref)):
        loads[f].wait()
        x = ref[0].astype(F32)
        stage[f] = x
        xt = x.T
        at = 2 * tips * f
        bands[lev, panel, at : at + STEPS] = x[:STEPS]
        bands[lev, panel, at + STEPS : at + tips] = x[width - STEPS :]
        bands[lev, panel, at + tips : at + tips + STEPS] = xt[:STEPS]
        bands[lev, panel, at + tips + STEPS : at + 2 * tips] = xt[width - STEPS :]
    for load in loads[3:6]:
        load.wait()
    facts, spread = slot_rows(
        col_ref[...], time_ref[...], count_ref[0], panels, area, width, capacity)
    bands[lev, panel, base : base + FACTS] = facts[:FACTS]
    hailed(near)
    started = []

    def remote(src, dst, ssem, rsem, where):
        return pltpu.make_async_remote_copy(
            src_ref=src, dst_ref=dst, send_sem=ssem, recv_sem=rsem,
            device_id=where, device_id_type=MESH)

    def send(src, dst, ssem, rsem, where):
        copy = remote(src, dst, ssem, rsem, where)
        copy.start()
        started.append(copy)
        return copy

    def block(level, at):
        return bands.at[level, at * subs + sub]

    arrivals_x, arrivals_c = [], []
    across = {"lev": other}

    def to_subs(level, at, k):
        for q in range(1, subs):
            arrivals_c.append(send(block(level, at), block(level, at), csend.at[q, level, k], crecv.at[q, level, at],
                                   {"sub": lax.rem(sub + q, subs)}))

    def to_lev(at, k):
        arrivals_x.append(send(block(lev, at), block(lev, at), xsend.at[k], xrecv.at[at], across))

    order = by_distance(tile, tiles)
    sends = list(enumerate(order))[::-1]
    for k, at in sends:
        send(block(lev, tile), block(lev, tile), zsend.at[k], zrecv.at[tile], {"tile": at})
    to_lev(tile, 0)
    to_subs(lev, tile, 0)
    fields = send(stage.at[:, pl.ds(ostart, rows)], win.at[lev], fsend, frecv, across)
    for f in range(3):
        win[lev, f] = stage[f, pl.ds(start, rows)]
    for load in loads[6:]:
        load.wait()
    jmine[...] = jac_ref[...].astype(F32)
    partner = partner_rows(pair_ref, flip_ref, levs, panels)
    e8 = jnp.broadcast_to(err_ref[...][None, :], (8, channels))
    high = lax.Precision.HIGHEST

    def slotted(g):
        a, b = halves(g)
        both = jnp.concatenate([a, b], axis=0).astype(BF16)
        out = dot(both, spread, NT)
        return out[:1] + out[8:9]

    gall[lev, panel, 0:1] = slotted(dot(e8, jmine[...] * jmine[...], NT, high))
    for k, at in enumerate(order):
        remote(block(lev, at), block(lev, at), zsend.at[k], zrecv.at[at], {"tile": at}).wait_recv()
        to_lev(at, k + 1)
        to_subs(lev, at, k + 1)
    jcopy = send(jmine.at[pl.ds(pl.multiple_of(other * share, MARGIN), share)], jother, jsend, jrecv, across)
    for k, at in enumerate([tile] + order):
        remote(block(other, at), block(other, at), xsend.at[k], xrecv.at[at], across).wait_recv()
        to_subs(other, at, k)
    fields.wait_recv()
    for level in (lev, other):
        for q in range(1, subs):
            for at in [tile] + order:
                whence = bands.at[level, at * subs + lax.rem(sub + q, subs)]
                remote(whence, whence, csend.at[q, level, 0], crecv.at[q, level, at],
                       {"sub": lax.rem(sub + q, subs)}).wait_recv()

    def band(f, which):
        at = (2 * f + which) * tips
        return bands[:, :, at : at + tips, :]

    def coefs(m, u, v):
        return (m + 0.5 * u, m - 0.5 * u, m + 0.5 * v, m - 0.5 * v)

    m4, v4 = per_level(dif_ref, levs, 4), per_level(ver_ref, levs, 4)
    m3, v3 = per_level(dif_ref, levs, 3), per_level(ver_ref, levs, 3)
    ns = coefs(m4, band(1, 0), band(2, 0))
    we = swap(coefs(m4, band(1, 1), band(2, 1)))
    own = coefs(m3, win[:, 1], win[:, 2])
    scal4 = (1.0 - 4.0 * m4 - 2.0 * v4, v4)
    scal3 = (1.0 - 4.0 * m3 - 2.0 * v3, v3)
    hit4 = edge_index((tips, width), tips, width) == iota((tips, width), 1)
    hit3 = iota((rows, width), 0) + start == iota((rows, width), 1)
    x_ns, x_we, x = band(0, 0), band(0, 1), win[:, 0]

    o_i, o_j, o_t = [by_panel(bands[0, :, base + k, :], capacity) for k in range(FACTS)]
    for k, v in enumerate((o_i, o_j, o_t)):
        box[k] = v
    s_i, s_j, s_t = [box[k, pl.ds(panel, 1), :] for k in range(FACTS)]
    line = iota((rows, width), 0)
    mine = (line + start + 1).astype(F32) == s_i
    inside = jnp.where((line >= lev * MARGIN) & (line < lev * MARGIN + half), 1.0, 0.0)
    here = jnp.where(mine, inside, 0.0)
    picked = [None] * levs
    for step in range(STEPS):
        strips = (x_ns[:, :, :1], x_ns[:, :, last:], x_we[:, :, :1], x_we[:, :, last:])
        h, ho = exchange(strips, store.at[step % 2], partner, panel)
        x = forward_tile(x, own, *scal3, ho, hit3)
        if step + 1 < STEPS:
            x_ns, x_we = (
                forward_tile(x_ns, ns, *scal4, h, hit4),
                forward_tile(x_we, we, *scal4, swap(h), hit4),
            )
        now = jnp.where(s_t == step + 1.0, here, 0.0)
        now = jnp.concatenate([now, now], axis=0).astype(BF16)
        for l in range(levs):
            got = dot(jnp.concatenate(halves(x[l]), axis=0).astype(BF16), now, TN)
            picked[l] = got if picked[l] is None else picked[l] + got
        if step == 1:
            jcopy.wait_recv()
            cross = dot(e8, jmine[pl.ds(pl.multiple_of(lev * share, MARGIN), share)] * jother[...], NT, high)
            cross = jnp.concatenate([cross] * levs, axis=1)
            cross = jnp.where(iota(cross.shape, 1) // share == lev, cross, 0.0)
            gall[lev, panel, 1:2] = slotted(cross)
            arrivals_g = [
                send(gall.at[lev, panel], gall.at[lev, panel], gsend.at[k], grecv.at[k], where)
                for k, where in enumerate(flat_peers)
            ]
    at_j = fiota((width, width), 0) + 1.0 == s_j
    for l in range(levs):
        vall[lev, panel, l : l + 1] = jnp.sum(jnp.where(at_j, picked[l], 0.0), axis=0, keepdims=True)
    arrivals_v = [
        send(vall.at[lev, panel], vall.at[lev, panel], vsend.at[k], vrecv.at[k], where)
        for k, where in enumerate(flat_peers)
    ]

    rcopy = send(res_ref.at[0, pl.ds(omid, half)], rother, rsend, rrecv, across)
    edge = edge_index((tips, width), tips, width).astype(F32) + 1.0
    spots = fiota((width, width), 0) + 1.0

    def onehots(p, a, b):
        tip = jnp.concatenate(
            [jnp.where((edge == a[p : p + 1]) & (o_t[p : p + 1] == t), 1.0, 0.0)
             for t in range(1, STEPS + 1)], axis=0)
        along = jnp.where(spots == b[p : p + 1], 1.0, 0.0)
        return tip, jnp.concatenate([along, along], axis=1).astype(BF16)

    hot_ns = [onehots(p, o_i, o_j) for p in range(panels)]
    hot_we = [onehots(p, o_j, o_i) for p in range(panels)]
    rows_own = jnp.concatenate(
        [jnp.where(mine & (s_t == t), 1.0, 0.0) for t in range(1, STEPS + 1)], axis=0)
    rows_own = jnp.concatenate([rows_own, rows_own], axis=1).astype(BF16)
    for copy in arrivals_g:
        copy.wait_recv()
    gram = {(l, l): by_panel(gall[l, :, 0, :], capacity) for l in range(levs)}
    gram[0, 1] = gram[1, 0] = by_panel(gall[0, :, 1, :] + gall[1, :, 1, :], capacity)
    for copy in arrivals_v:
        copy.wait_recv()
    total = vall[0] + vall[1]
    back = [gram[a, 0] * total[:, 0] + gram[a, 1] * total[:, 1] for a in range(levs)]
    parts = [halves(b) for b in back]

    def band_forcing(hot):
        out = []
        for p in range(panels):
            tip, along = hot[p]
            left = jnp.concatenate(
                [jnp.concatenate([tip * v[p : p + 1] for v in parts[l]], axis=1) for l in range(levs)],
                axis=0)
            out.append(dot(left.astype(BF16), along, NT))
        return [
            jnp.stack([
                jnp.stack([o[(l * STEPS + t) * tips : (l * STEPS + t + 1) * tips] for o in out])
                for l in range(levs)])
            for t in range(STEPS)
        ]

    for l in range(levs):
        box[l] = back[l]
    scaled = []
    for l in range(levs):
        v = halves(box[l, pl.ds(panel, 1), :])
        scaled.append(jnp.concatenate([jnp.where(at_j, w, 0.0) for w in v], axis=1))
    flat = dot(rows_own, jnp.concatenate(scaled, axis=0).astype(BF16), NT)
    force = [
        jnp.stack([flat[t * rows : (t + 1) * rows, l * width : (l + 1) * width] for l in range(levs)])
        for t in range(STEPS)
    ]
    force_ns, force_we = band_forcing(hot_ns), band_forcing(hot_we)
    x, x_ns, x_we = force[-1], force_ns[-1], force_we[-1]
    for step in range(STEPS - 1, -1, -1):
        p_ns = [c * x_ns for c in ns]
        p_we = [c * x_we for c in we]
        strips = (p_ns[0][:, :, :1], p_ns[1][:, :, last:], p_we[0][:, :, :1], p_we[1][:, :, last:])
        h, ho = exchange(strips, store.at[step % 2], partner, panel)
        x = adjoint_tile(x, [c * x for c in own], *scal3, ho, hit3)
        if step > 0:
            x = x + force[step - 1]
            x_ns = adjoint_tile(x_ns, p_ns, *scal4, h, hit4) + force_ns[step - 1]
            x_we = adjoint_tile(x_we, p_we, *scal4, swap(h), hit4) + force_we[step - 1]

    rcopy.wait_recv()
    x = jnp.where(lev == 0, x[:, :half], x[:, rows - half :])
    direction = [win[l, 0, pl.ds(pl.multiple_of(lev * MARGIN, MARGIN), half)] for l in range(levs)]
    image = [x[l] + inv_ref[l] * direction[l] for l in range(levs)]
    own_res, other_res = res_ref[0, pl.ds(mid, half)], rother[...]
    sums = None
    for l in range(levs):
        res = jnp.where(lev == l, own_res, other_res)
        pairs = ((res, res), (direction[l], image[l]), (res, image[l]), (image[l], image[l]))
        part = jnp.concatenate([jnp.sum(a * b, axis=0, keepdims=True) for a, b in pairs], axis=0)
        sums = part if sums is None else sums + part
    sall[me] = sums
    arrivals_s = [
        send(sall.at[me], sall.at[me], ssend.at[k], srecv.at[k], where)
        for k, where in enumerate(flat_peers)
    ]
    isent[...] = jnp.where(lev == 0, image[1], image[0])
    icopy = send(isent, igot, isend, irecv, across)
    img_out[0, pl.ds(mid, half)] = jnp.where(lev == 0, image[0], image[1])
    icopy.wait_recv()
    img_out[0, pl.ds(omid, half)] = igot[...]
    for copy in arrivals_s:
        copy.wait_recv()
    total = jnp.sum(jnp.sum(sall[...], axis=0), axis=1, keepdims=True)
    old, curvature, cross, square = [total[k : k + 1] for k in range(4)]
    alpha = old / curvature
    new = old - 2.0 * alpha * cross + alpha * alpha * square
    alpha_out[0] = jnp.broadcast_to(alpha, alpha_out.shape[1:])
    beta_out[0] = jnp.broadcast_to(new / old, beta_out.shape[1:])
    for copy in started:
        copy.wait_send()


def fused_body(
    increment, residual, direction, wind_u, wind_v, diffusion, vertical, background_inv,
    side_pair, side_flip, obs_column, obs_time, obs_count, jacobian, error_inv,
):
    sizes = grid_sizes()
    tiles, levs, subs = sizes
    panels = tiles * subs
    everyone = panels * levs
    width = increment.shape[2]
    slots, _, channels = jacobian.shape
    half = width // levs
    rows = half + MARGIN
    dma = pltpu.SemaphoreType.DMA
    inputs = (
        direction, wind_u, wind_v, obs_column[None, :], obs_time[None, :], obs_count,
        jacobian.reshape(slots, channels), error_inv, side_pair.T, side_flip.T, diffusion, vertical,
        background_inv, residual,
    )
    scalars = (5, 8, 9, 10, 11, 12)
    landing = [
        (pltpu.SMEM if k in scalars else pltpu.VMEM)(x.shape, x.dtype) for k, x in enumerate(inputs)
    ]
    row = jax.ShapeDtypeStruct((1, 1, width), F32)
    image, alpha, beta = pl.pallas_call(
        functools.partial(whole_kernel, sizes, slot_capacity(slots, panels)),
        out_shape=(jax.ShapeDtypeStruct(increment.shape, F32), row, row),
        in_specs=[pl.BlockSpec(memory_space=pl.ANY)] * len(inputs),
        out_specs=(VM, VM, VM),
        scratch_shapes=landing + [
            dma((len(inputs),)),
            pltpu.VMEM((3, width, width), F32),
            pltpu.VMEM((levs, 3, rows, width), F32),
            pltpu.VMEM((levs, panels, 12 * STEPS + FACTS, width), F32),
            pltpu.VMEM((slots, channels), F32),
            pltpu.VMEM((slots // levs, channels), F32),
            pltpu.VMEM((levs, panels, 2, width), F32),
            pltpu.VMEM((levs, panels, levs, width), F32),
            pltpu.VMEM((everyone, 4, width), F32),
            pltpu.VMEM((half, width), F32),
            pltpu.VMEM((half, width), F32),
            pltpu.VMEM((half, width), F32),
            pltpu.VMEM((2, 2 * levs * 4 * panels, width), F32),
            pltpu.VMEM((FACTS, panels, width), F32),
            dma, dma,
            dma((tiles,)), dma((tiles,)),
            dma((tiles,)), dma((tiles,)),
            dma((subs, levs, tiles)), dma((subs, levs, tiles)),
            dma, dma,
            dma, dma,
            dma, dma,
            dma((everyone,)), dma((everyone,)),
            dma((everyone,)), dma((everyone,)),
            dma((everyone,)), dma((everyone,)),
        ],
        compiler_params=pltpu.CompilerParams(
            collective_id=0, has_side_effects=True, vmem_limit_bytes=16 * 1024 * 1024),
        name="whole",
    )(*[x if x.size == 1 else pltpu.with_memory_space_constraint(x, pltpu.HBM) for x in inputs])
    left = residual - alpha * image
    return increment + alpha * direction, left, left + beta * direction


def chosen(*args):
    tiles, levs, subs = grid_sizes()
    increment, jacobian = args[0], args[13]
    width, slots, panels = increment.shape[2], jacobian.shape[0], tiles * subs
    fits = (
        levs == 2
        and increment.shape[0] == 1
        and increment.shape[1] == width
        and panels * slot_capacity(slots, panels) == width
        and panels == 8
        and slots % (8 * levs) == 0
        and width % (8 * levs) == 0
        and STEPS <= MARGIN
        and width >= 2 * STEPS
    )
    return fused_body(*args) if fits else body(*args)


def solution(mesh):
    placed = (
        P(("member", "lev"), ("tile", "sub"), None),
        P(("member", "lev"), ("tile", "sub"), None),
        P(("member", "lev"), ("tile", "sub"), None),
        P(("member", "lev"), ("tile", "sub"), None),
        P(("member", "lev"), ("tile", "sub"), None),
        P(),
        P(),
        P(),
        P(),
        P(),
        P(("tile", "sub")),
        P(("tile", "sub")),
        P(("tile", "sub")),
        P(("tile", "sub"), "lev", None),
        P(),
    )
    return jax.shard_map(
        chosen,
        mesh=mesh,
        in_specs=placed,
        out_specs=(
            P(("member", "lev"), ("tile", "sub"), None),
            P(("member", "lev"), ("tile", "sub"), None),
            P(("member", "lev"), ("tile", "sub"), None),
        ),
        check_vma=False,
    )
```

```python
import jax
import jax.numpy as jnp
from jax import lax
from jax.experimental import pallas as pl
from jax.experimental.pallas import tpu as pltpu
import functools
from jax.sharding import PartitionSpec as P

STEPS = 4


def with_halo(block, sides, width):
    for axis, dim in sides:
        count = lax.axis_size(axis)
        forward = [(i, i + 1) for i in range(count - 1)]
        backward = [(target, source) for source, target in forward]
        low = lax.ppermute(
            lax.slice_in_dim(block, block.shape[dim] - width, None, axis=dim), axis, forward
        )
        high = lax.ppermute(lax.slice_in_dim(block, 0, width, axis=dim), axis, backward)
        block = jnp.concatenate([low, block, high], axis=dim)
    return block


def neighbours(strips, pair_rows, flip_rows):
    everyone = lax.all_gather(strips, ("tile", "sub"), axis=0, tiled=True)
    picked = everyone[pair_rows]
    return jnp.where(flip_rows[:, None, None] == 1, picked[:, :, ::-1], picked)


def level_padded(field):
    return with_halo(field, (("lev", 0),), 1)


def body(
    increment,
    residual,
    direction,
    wind_u,
    wind_v,
    diffusion,
    vertical,
    background_inv,
    side_pair,
    side_flip,
    obs_column,
    obs_time,
    obs_count,
    jacobian,
    error_inv,
):
    depth = increment.shape[0]
    width = increment.shape[2]
    slots = obs_column.shape[0]
    panels = lax.axis_size(("tile", "sub"))
    capacity = max(2, (2 * slots + panels - 1) // panels)
    panel = lax.axis_index(("tile", "sub"))
    first_level = lax.axis_index("lev") * depth
    mixing = lax.dynamic_slice_in_dim(diffusion, first_level, depth)[:, None, None]
    blending = lax.dynamic_slice_in_dim(vertical, first_level, depth)[:, None, None]
    prior = lax.dynamic_slice_in_dim(background_inv, first_level, depth)[:, None, None]
    pair_rows = lax.dynamic_index_in_dim(side_pair, panel, 0, keepdims=False)
    flip_rows = lax.dynamic_index_in_dim(side_flip, panel, 0, keepdims=False)
    speed_u = wind_u.astype(jnp.float32)
    speed_v = wind_v.astype(jnp.float32)
    coefs = (
        mixing + 0.5 * speed_u,
        mixing - 0.5 * speed_u,
        mixing + 0.5 * speed_v,
        mixing - 0.5 * speed_v,
    )
    center = 1.0 - 4.0 * mixing - 2.0 * blending

    def forward(field):
        strips = jnp.stack([field[:, 0, :], field[:, -1, :], field[:, :, 0], field[:, :, -1]])
        halos = neighbours(strips, pair_rows, flip_rows)
        north = jnp.concatenate([halos[0][:, None, :], field[:, :-1, :]], axis=1)
        south = jnp.concatenate([field[:, 1:, :], halos[1][:, None, :]], axis=1)
        west = jnp.concatenate([halos[2][:, :, None], field[:, :, :-1]], axis=2)
        east = jnp.concatenate([field[:, :, 1:], halos[3][:, :, None]], axis=2)
        padded = level_padded(field)
        return (
            center * field
            + coefs[0] * north
            + coefs[1] * south
            + coefs[2] * west
            + coefs[3] * east
            + blending * (padded[:-2] + padded[2:])
        )

    def adjoint(field):
        prods = [c * field for c in coefs]
        strips = jnp.stack(
            [prods[0][:, 0, :], prods[1][:, -1, :], prods[2][:, :, 0], prods[3][:, :, -1]]
        )
        halos = neighbours(strips, pair_rows, flip_rows)
        rows_term = jnp.concatenate([prods[0][:, 1:, :], halos[1][:, None, :]], axis=1)
        rows_term = rows_term + jnp.concatenate([halos[0][:, None, :], prods[1][:, :-1, :]], axis=1)
        cols_term = jnp.concatenate([prods[2][:, :, 1:], halos[3][:, :, None]], axis=2)
        cols_term = cols_term + jnp.concatenate([halos[2][:, :, None], prods[3][:, :, :-1]], axis=2)
        padded = level_padded(blending * field)
        return center * field + rows_term + cols_term + padded[:-2] + padded[2:]

    state = direction
    states = []
    for step in range(STEPS):
        state = forward(state)
        states.append(state.reshape(depth, width * width))
    history = jnp.stack(states, axis=0)
    area = width * width
    alive = jnp.arange(slots, dtype=jnp.int32) < obs_count[0]
    targets = obs_column // area
    cells = obs_column % area
    owned = (
        (targets[:, None] == jnp.arange(panels, dtype=jnp.int32)[None, :]) & alive[:, None]
    ).astype(jnp.int32)
    rank = jnp.sum((jnp.cumsum(owned, axis=0) - owned) * owned, axis=1)
    position = jnp.where(alive, targets * capacity + rank, panels * capacity)
    want_cell = (
        jnp.zeros((panels * capacity,), jnp.int32)
        .at[position]
        .set(cells, mode="drop")
        .reshape(panels, capacity)
    )
    want_time = (
        jnp.ones((panels * capacity,), jnp.int32)
        .at[position]
        .set(obs_time, mode="drop")
        .reshape(panels, capacity)
    )
    asked_cell = lax.all_to_all(want_cell, ("tile", "sub"), split_axis=0, concat_axis=0, tiled=True)
    asked_time = lax.all_to_all(want_time, ("tile", "sub"), split_axis=0, concat_axis=0, tiled=True)
    values = history[asked_time - 1, :, asked_cell]
    sent = lax.all_to_all(values, ("tile", "sub"), split_axis=0, concat_axis=0, tiled=True)
    gathered = sent.reshape(panels * capacity, depth)[jnp.minimum(position, panels * capacity - 1)]
    wide = jacobian.astype(jnp.float32)
    partial_value = jnp.einsum("olc,ol->oc", wide, gathered, precision=lax.Precision.HIGHEST)
    departure = lax.psum(partial_value, "lev")
    weighted = departure * error_inv[None, :]
    back = jnp.einsum("olc,oc->ol", wide, weighted, precision=lax.Precision.HIGHEST)
    back = back * alive.astype(jnp.float32)[:, None]
    outgoing = (
        jnp.zeros((panels * capacity, depth), jnp.float32)
        .at[position]
        .set(back, mode="drop")
        .reshape(panels, capacity, depth)
    )
    incoming = lax.all_to_all(outgoing, ("tile", "sub"), split_axis=0, concat_axis=0, tiled=True)
    flat_cell = asked_cell.reshape(panels * capacity)
    flat_time = asked_time.reshape(panels * capacity) - 1
    forcing = (
        jnp.zeros((STEPS, depth, area), jnp.float32)
        .at[flat_time, :, flat_cell]
        .add(incoming.reshape(panels * capacity, depth))
    )
    forcing = forcing.reshape(STEPS, depth, width, width)
    sensitivity = forcing[STEPS - 1]
    for step in range(STEPS - 1, 0, -1):
        sensitivity = adjoint(sensitivity) + forcing[step - 1]
    sensitivity = adjoint(sensitivity)
    image = prior * direction + sensitivity
    norm_old, curvature, cross, square = lax.psum(
        (
            jnp.sum(residual * residual),
            jnp.sum(direction * image),
            jnp.sum(residual * image),
            jnp.sum(image * image),
        ),
        ("tile", "lev", "sub"),
    )
    alpha = norm_old / curvature
    increment_new = increment + alpha * direction
    residual_new = residual - alpha * image
    norm_new = norm_old - 2.0 * alpha * cross + alpha * alpha * square
    direction_new = residual_new + norm_new / norm_old * direction
    return (increment_new, residual_new, direction_new)


MESH = pl.DeviceIdType.MESH
VM = pl.BlockSpec(memory_space=pltpu.VMEM)
F32 = jnp.float32
BF16 = jnp.bfloat16
NT = (((1,), (1,)), ((), ()))
TN = (((0,), (0,)), ((), ()))
NN = (((1,), (0,)), ((), ()))
FACTS = 3
MARGIN = 8
INPUTS = 14


def grid_sizes():
    return lax.axis_size("tile"), lax.axis_size("lev"), lax.axis_size("sub")


def slot_capacity(slots, panels):
    return max(2, (2 * slots + panels - 1) // panels)


def hail(peers):
    barrier = pltpu.get_barrier_semaphore()
    for peer in peers:
        pl.semaphore_signal(barrier, inc=1, device_id=peer, device_id_type=MESH)


def hailed(peers):
    pl.semaphore_wait(pltpu.get_barrier_semaphore(), len(peers))


def group_peers(sizes):
    axes = ("tile", "lev", "sub")
    steps = [(t, l, u) for t in range(sizes[0]) for l in range(sizes[1]) for u in range(sizes[2])]
    steps.sort(key=lambda d: (-min(d[0], sizes[0] - d[0]), -d[1], -d[2]))
    return [
        {axis: lax.rem(lax.axis_index(axis) + by, size) for axis, by, size in zip(axes, d, sizes)}
        for d in steps if any(d)
    ]


def by_distance(tile, tiles):
    table = [sorted((t for t in range(tiles) if t != me), key=lambda t: abs(t - me)) for me in range(tiles)]
    picks = []
    for k in range(tiles - 1):
        pick = jnp.int32(table[0][k])
        for me in range(1, tiles):
            pick = jnp.where(tile == me, table[me][k], pick)
        picks.append(pick)
    return picks


def dot(a, b, dims, precision=None):
    return lax.dot_general(a, b, dims, precision=precision, preferred_element_type=F32)


def iota(shape, axis):
    return lax.broadcasted_iota(jnp.int32, shape, axis)


def fiota(shape, axis):
    return iota(shape, axis).astype(F32)


def halves(x):
    high = x.astype(BF16).astype(F32)
    return high, x - high


def per_level(ref, levels, ndim):
    return jnp.stack([jnp.full((1,) * (ndim - 1), ref[l], F32) for l in range(levels)])


def edge_index(shape, rows, width):
    r = iota(shape, len(shape) - 2)
    return jnp.where(r < rows // 2, r, r + (width - rows))


def column_of(halo, hit):
    return jnp.sum(jnp.where(hit, halo, 0.0), axis=-1, keepdims=True)


def shifted(x, axis, by, edge):
    n = x.shape[axis]
    rolled = pltpu.roll(x, by % n, axis)
    place_of = iota(x.shape[-2:], axis - (x.ndim - 2))
    return jnp.where(place_of == (0 if by == 1 else n - 1), edge, rolled)


def vertical_sum(x):
    levels = x.shape[0]
    parts = []
    for l in range(levels):
        total = jnp.zeros_like(x[l])
        if l > 0:
            total = total + x[l - 1]
        if l + 1 < levels:
            total = total + x[l + 1]
        parts.append(total)
    return jnp.stack(parts)


def forward_tile(x, c, center, vert, h, hit):
    r, w = x.ndim - 2, x.ndim - 1
    return (
        center * x
        + c[0] * shifted(x, r, 1, h[0])
        + c[1] * shifted(x, r, -1, h[1])
        + c[2] * shifted(x, w, 1, column_of(h[2], hit))
        + c[3] * shifted(x, w, -1, column_of(h[3], hit))
        + vert * vertical_sum(x)
    )


def adjoint_tile(x, p, center, vert, h, hit):
    r, w = x.ndim - 2, x.ndim - 1
    return (
        center * x
        + shifted(p[0], r, -1, h[1])
        + shifted(p[1], r, 1, h[0])
        + shifted(p[2], w, -1, column_of(h[3], hit))
        + shifted(p[3], w, 1, column_of(h[2], hit))
        + vertical_sum(vert * x)
    )


def swap(q):
    return (q[2], q[3], q[0], q[1])


def turned(x):
    width = x.shape[1]
    back = width - 1 - iota((8, width), 1)
    return jnp.concatenate(
        [jnp.take_along_axis(x[r : r + 8], back, axis=1) for r in range(0, x.shape[0], 8)], axis=0)


def partner_rows(pair_ref, flip_ref, levels, panels):
    sides = 4 * panels

    def row(k, p):
        pair = pair_ref[k, p]
        return (flip_ref[k, p] * levels * sides) + (pair % 4) * panels + pair // 4

    return row


def exchange(strips, store, row, panel):
    levels, panels, _, width = strips[0].shape
    sides = 4 * panels
    s = jnp.concatenate(
        [strips[k][l].reshape(panels, width) for l in range(levels) for k in range(4)], axis=0)
    store[: levels * sides] = s
    store[levels * sides :] = turned(s)

    def strip(k, p, l):
        return store[pl.ds(row(k, p) + l * sides, 1), :]

    every = [
        jnp.stack([jnp.stack([strip(k, p, l) for p in range(panels)]) for l in range(levels)])
        for k in range(4)
    ]
    return every, [jnp.stack([strip(k, panel, l) for l in range(levels)]) for k in range(4)]


def slot_rows(col, when, count, panels, area, width, capacity):
    slots = col.shape[1]
    alive = iota((1, slots), 1) < count
    panel = jnp.where(alive, col // area, -1)
    cell = col % area
    owned = (iota((panels, slots), 0) == panel).astype(F32)
    earlier = (iota((slots, slots), 0) < iota((slots, slots), 1)).astype(BF16)
    rank = jnp.sum(owned * dot(owned.astype(BF16), earlier, NN), axis=0, keepdims=True)
    slot = jnp.where(alive, panel.astype(F32) * capacity + rank, -1.0)
    spread = (fiota((panels * capacity, slots), 0) == slot).astype(BF16)
    facts = jnp.concatenate([cell // width + 1, cell % width + 1, when], axis=0).astype(F32)
    facts = jnp.concatenate([facts, jnp.zeros((8 - FACTS, slots), F32)], axis=0)
    tall = jnp.concatenate([slot, jnp.zeros((7, slots), F32)], axis=0).T
    upright = (fiota((slots, panels * capacity), 1) == tall[:, 0:1]).astype(F32)
    return dot(facts.astype(BF16), spread, NT), spread, upright


def by_panel(a, capacity):
    owners, width = a.shape
    mine = iota((owners, width), 1) // capacity == iota((owners, width), 0)
    slanted = pltpu.roll(a, 0, 1, stride=capacity, stride_axis=0)
    rows = []
    for p in range(width // capacity):
        r = pltpu.roll(slanted, width - p * capacity, 1) if p else slanted
        rows.append(jnp.sum(jnp.where(mine, r, 0.0), axis=0, keepdims=True))
    return jnp.concatenate(rows, axis=0)


def whole_kernel(sizes, capacity, *refs):
    tiles, levs, subs = sizes
    inputs, (img_out, alpha_out, beta_out) = refs[:INPUTS], refs[INPUTS : INPUTS + 3]
    held = refs[INPUTS + 3 : 2 * INPUTS + 3]
    (landed, stage, win, bands, jmine, jother, gall, vall, sall, rother, isent, igot, store, box, upright,
     fsend, frecv, zsend, zrecv, xsend, xrecv, csend, crecv, jsend, jrecv, rsend, rrecv, isend, irecv,
     gsend, grecv, vsend, vrecv, ssend, srecv) = refs[2 * INPUTS + 3 :]
    (dir_ref, wu_ref, wv_ref, col_ref, time_ref, count_ref, jac_ref, err_ref, pair_ref, flip_ref,
     dif_ref, ver_ref, inv_ref, res_ref) = held
    loads = [
        pltpu.make_async_copy(src, dst, landed.at[k]) for k, (src, dst) in enumerate(zip(inputs, held))
    ]
    flat_peers = group_peers(sizes)
    near = [{axis: lax.rem(lax.axis_index(axis) + k, size)}
            for axis, size in zip(("tile", "lev", "sub"), sizes) for k in range(1, size)]
    hail(near)
    for load in loads[:6]:
        load.start()
    for load in loads[6:]:
        load.start()

    tile, lev, sub = lax.axis_index("tile"), lax.axis_index("lev"), lax.axis_index("sub")
    panels = tiles * subs
    panel = tile * subs + sub
    me = (tile * levs + lev) * subs + sub
    other = 1 - lev
    slots, channels = jac_ref.shape
    width = dir_ref.shape[2]
    area = width * width
    tips = 2 * STEPS
    last = tips - 1
    base = 6 * tips
    half = width // levs
    rows = half + MARGIN
    start = pl.multiple_of(lev * (width - rows), MARGIN)
    ostart = pl.multiple_of(other * (width - rows), MARGIN)
    mid = pl.multiple_of(lev * half, MARGIN)
    omid = pl.multiple_of(other * half, MARGIN)
    share = slots // levs

    for f, ref in enumerate((dir_ref, wu_ref, wv_ref)):
        loads[f].wait()
        x = ref[0].astype(F32)
        stage[f] = x
        xt = x.T
        at = 2 * tips * f
        bands[lev, panel, at : at + STEPS] = x[:STEPS]
        bands[lev, panel, at + STEPS : at + tips] = x[width - STEPS :]
        bands[lev, panel, at + tips : at + tips + STEPS] = xt[:STEPS]
        bands[lev, panel, at + tips + STEPS : at + 2 * tips] = xt[width - STEPS :]
    for load in loads[3:6]:
        load.wait()
    facts, spread, upright[...] = slot_rows(
        col_ref[...], time_ref[...], count_ref[0], panels, area, width, capacity)
    bands[lev, panel, base : base + FACTS] = facts[:FACTS]
    hailed(near)
    started = []

    def remote(src, dst, ssem, rsem, where):
        return pltpu.make_async_remote_copy(
            src_ref=src, dst_ref=dst, send_sem=ssem, recv_sem=rsem,
            device_id=where, device_id_type=MESH)

    def send(src, dst, ssem, rsem, where):
        copy = remote(src, dst, ssem, rsem, where)
        copy.start()
        started.append(copy)
        return copy

    def block(level, at):
        return bands.at[level, at * subs + sub]

    arrivals_x, arrivals_c = [], []
    across = {"lev": other}

    def to_subs(level, at, k):
        for q in range(1, subs):
            arrivals_c.append(send(block(level, at), block(level, at), csend.at[q, level, k], crecv.at[q, level, at],
                                   {"sub": lax.rem(sub + q, subs)}))

    def to_lev(at, k):
        arrivals_x.append(send(block(lev, at), block(lev, at), xsend.at[k], xrecv.at[at], across))

    order = by_distance(tile, tiles)
    sends = list(enumerate(order))[::-1]
    for k, at in sends:
        send(block(lev, tile), block(lev, tile), zsend.at[k], zrecv.at[tile], {"tile": at})
    to_lev(tile, 0)
    to_subs(lev, tile, 0)
    fields = send(stage.at[:, pl.ds(ostart, rows)], win.at[lev], fsend, frecv, across)
    for f in range(3):
        win[lev, f] = stage[f, pl.ds(start, rows)]
    for load in loads[6:]:
        load.wait()
    jmine[...] = jac_ref[...].astype(F32)
    partner = partner_rows(pair_ref, flip_ref, levs, panels)
    e8 = jnp.broadcast_to(err_ref[...][None, :], (8, channels))
    high = lax.Precision.HIGHEST

    def slotted(g):
        a, b = halves(g)
        both = jnp.concatenate([a, b], axis=0).astype(BF16)
        out = dot(both, spread, NT)
        return out[:1] + out[8:9]

    gall[lev, panel, 0:1] = slotted(dot(e8, jmine[...] * jmine[...], NT, high))
    for k, at in enumerate(order):
        remote(block(lev, at), block(lev, at), zsend.at[k], zrecv.at[at], {"tile": at}).wait_recv()
        to_lev(at, k + 1)
        to_subs(lev, at, k + 1)

    def from_sub(level):
        for q in range(1, subs):
            for at in [tile] + order:
                whence = bands.at[level, at * subs + lax.rem(sub + q, subs)]
                remote(whence, whence, csend.at[q, level, 0], crecv.at[q, level, at],
                       {"sub": lax.rem(sub + q, subs)}).wait_recv()

    from_sub(lev)
    jcopy = send(jmine.at[pl.ds(pl.multiple_of(other * share, MARGIN), share)], jother, jsend, jrecv, across)
    for k, at in enumerate([tile] + order):
        remote(block(other, at), block(other, at), xsend.at[k], xrecv.at[at], across).wait_recv()
        to_subs(other, at, k)

    o_i, o_j, o_t = [by_panel(bands[lev, :, base + k, :], capacity) for k in range(FACTS)]
    for k, v in enumerate((o_i, o_j, o_t)):
        box[k] = v
    s_i, s_j, s_t = [box[k, pl.ds(panel, 1), :] for k in range(FACTS)]
    line = iota((rows, width), 0)
    mine = (line + start + 1).astype(F32) == s_i
    inside = jnp.where((line >= lev * MARGIN) & (line < lev * MARGIN + half), 1.0, 0.0)
    here = jnp.where(mine, inside, 0.0)
    fields.wait_recv()
    from_sub(other)

    def band(f, which):
        at = (2 * f + which) * tips
        return bands[:, :, at : at + tips, :]

    def coefs(m, u, v):
        return (m + 0.5 * u, m - 0.5 * u, m + 0.5 * v, m - 0.5 * v)

    m4, v4 = per_level(dif_ref, levs, 4), per_level(ver_ref, levs, 4)
    m3, v3 = per_level(dif_ref, levs, 3), per_level(ver_ref, levs, 3)
    ns = coefs(m4, band(1, 0), band(2, 0))
    we = swap(coefs(m4, band(1, 1), band(2, 1)))
    own = coefs(m3, win[:, 1], win[:, 2])
    scal4 = (1.0 - 4.0 * m4 - 2.0 * v4, v4)
    scal3 = (1.0 - 4.0 * m3 - 2.0 * v3, v3)
    hit4 = edge_index((tips, width), tips, width) == iota((tips, width), 1)
    hit3 = iota((rows, width), 0) + start == iota((rows, width), 1)
    x_ns, x_we, x = band(0, 0), band(0, 1), win[:, 0]

    at_j = fiota((width, width), 0) + 1.0 == s_j
    pick_j = jnp.where(at_j, 1.0, 0.0)
    pick_j = jnp.concatenate([pick_j, pick_j], axis=0).astype(BF16)
    picked = jnp.zeros((levs, rows, width), F32)
    for step in range(STEPS):
        strips = (x_ns[:, :, :1], x_ns[:, :, last:], x_we[:, :, :1], x_we[:, :, last:])
        h, ho = exchange(strips, store.at[step % 2], partner, panel)
        x = forward_tile(x, own, *scal3, ho, hit3)
        if step + 1 < STEPS:
            x_ns, x_we = (
                forward_tile(x_ns, ns, *scal4, h, hit4),
                forward_tile(x_we, we, *scal4, swap(h), hit4),
            )
        now = jnp.where(s_t == step + 1.0, here, 0.0)
        both = jnp.concatenate([jnp.concatenate(halves(x[l]), axis=1) for l in range(levs)], axis=0)
        picked = picked + now * dot(both.astype(BF16), pick_j, NN).reshape(levs, rows, width)
        if step == 1:
            jcopy.wait_recv()
            near_half = pl.multiple_of(lev * share, MARGIN)
            cross = jmine[pl.ds(near_half, share)] * jother[...] * err_ref[...][None, :]
            cross = jnp.sum(cross, axis=1, keepdims=True) * upright[pl.ds(near_half, share)]
            gall[lev, panel, 1:2] = jnp.sum(cross, axis=0, keepdims=True)
            arrivals_g = [
                send(gall.at[lev, panel], gall.at[lev, panel], gsend.at[k], grecv.at[k], where)
                for k, where in enumerate(flat_peers)
            ]
    for l in range(levs):
        vall[lev, panel, l : l + 1] = jnp.sum(picked[l], axis=0, keepdims=True)
    arrivals_v = [
        send(vall.at[lev, panel], vall.at[lev, panel], vsend.at[k], vrecv.at[k], where)
        for k, where in enumerate(flat_peers)
    ]

    rcopy = send(res_ref.at[0, pl.ds(omid, half)], rother, rsend, rrecv, across)
    edge = edge_index((tips, width), tips, width).astype(F32) + 1.0
    spots = fiota((width, width), 0) + 1.0

    def onehots(p, a, b):
        tip = jnp.concatenate(
            [jnp.where((edge == a[p : p + 1]) & (o_t[p : p + 1] == t), 1.0, 0.0)
             for t in range(1, STEPS + 1)], axis=0)
        along = jnp.where(spots == b[p : p + 1], 1.0, 0.0)
        return tip, jnp.concatenate([along, along], axis=1).astype(BF16)

    hot_ns = [onehots(p, o_i, o_j) for p in range(panels)]
    hot_we = [onehots(p, o_j, o_i) for p in range(panels)]
    rows_own = jnp.concatenate(
        [jnp.where(mine & (s_t == t), 1.0, 0.0) for t in range(1, STEPS + 1)], axis=0)
    rows_own = jnp.concatenate([rows_own, rows_own], axis=1).astype(BF16)
    for copy in arrivals_g:
        copy.wait_recv()
    gram = {(l, l): by_panel(gall[l, :, 0, :], capacity) for l in range(levs)}
    gram[0, 1] = gram[1, 0] = by_panel(gall[0, :, 1, :] + gall[1, :, 1, :], capacity)
    for copy in arrivals_v:
        copy.wait_recv()
    total = vall[0] + vall[1]
    back = [gram[a, 0] * total[:, 0] + gram[a, 1] * total[:, 1] for a in range(levs)]
    parts = [halves(b) for b in back]

    def band_forcing(hot):
        out = []
        for p in range(panels):
            tip, along = hot[p]
            left = jnp.concatenate(
                [jnp.concatenate([tip * v[p : p + 1] for v in parts[l]], axis=1) for l in range(levs)],
                axis=0)
            out.append(dot(left.astype(BF16), along, NT))
        return [
            jnp.stack([
                jnp.stack([o[(l * STEPS + t) * tips : (l * STEPS + t + 1) * tips] for o in out])
                for l in range(levs)])
            for t in range(STEPS)
        ]

    for l in range(levs):
        box[l] = back[l]
    scaled = []
    for l in range(levs):
        v = halves(box[l, pl.ds(panel, 1), :])
        scaled.append(jnp.concatenate([jnp.where(at_j, w, 0.0) for w in v], axis=1))
    flat = dot(rows_own, jnp.concatenate(scaled, axis=0).astype(BF16), NT)
    force = [
        jnp.stack([flat[t * rows : (t + 1) * rows, l * width : (l + 1) * width] for l in range(levs)])
        for t in range(STEPS)
    ]
    force_ns, force_we = band_forcing(hot_ns), band_forcing(hot_we)
    x, x_ns, x_we = force[-1], force_ns[-1], force_we[-1]
    for step in range(STEPS - 1, -1, -1):
        p_ns = [c * x_ns for c in ns]
        p_we = [c * x_we for c in we]
        strips = (p_ns[0][:, :, :1], p_ns[1][:, :, last:], p_we[0][:, :, :1], p_we[1][:, :, last:])
        h, ho = exchange(strips, store.at[step % 2], partner, panel)
        x = adjoint_tile(x, [c * x for c in own], *scal3, ho, hit3)
        if step > 0:
            x = x + force[step - 1]
            x_ns = adjoint_tile(x_ns, p_ns, *scal4, h, hit4) + force_ns[step - 1]
            x_we = adjoint_tile(x_we, p_we, *scal4, swap(h), hit4) + force_we[step - 1]

    rcopy.wait_recv()
    x = jnp.where(lev == 0, x[:, :half], x[:, rows - half :])
    direction = [win[l, 0, pl.ds(pl.multiple_of(lev * MARGIN, MARGIN), half)] for l in range(levs)]
    image = [x[l] + inv_ref[l] * direction[l] for l in range(levs)]
    own_res, other_res = res_ref[0, pl.ds(mid, half)], rother[...]
    sums = None
    for l in range(levs):
        res = jnp.where(lev == l, own_res, other_res)
        pairs = ((res, res), (direction[l], image[l]), (res, image[l]), (image[l], image[l]))
        part = jnp.concatenate([jnp.sum(a * b, axis=0, keepdims=True) for a, b in pairs], axis=0)
        sums = part if sums is None else sums + part
    sall[me] = sums
    before = list(started)
    arrivals_s = [
        send(sall.at[me], sall.at[me], ssend.at[k], srecv.at[k], where)
        for k, where in enumerate(flat_peers)
    ]
    isent[...] = jnp.where(lev == 0, image[1], image[0])
    icopy = send(isent, igot, isend, irecv, across)
    img_out[0, pl.ds(mid, half)] = jnp.where(lev == 0, image[0], image[1])
    for copy in before:
        copy.wait_send()
    icopy.wait_recv()
    img_out[0, pl.ds(omid, half)] = igot[...]
    for copy in arrivals_s:
        copy.wait_recv()
    total = jnp.sum(jnp.sum(sall[...], axis=0), axis=1, keepdims=True)
    old, curvature, cross, square = [total[k : k + 1] for k in range(4)]
    alpha = old / curvature
    new = old - 2.0 * alpha * cross + alpha * alpha * square
    alpha_out[0] = jnp.broadcast_to(alpha, alpha_out.shape[1:])
    beta_out[0] = jnp.broadcast_to(new / old, beta_out.shape[1:])
    for copy in started[len(before) :]:
        copy.wait_send()


def fused_body(
    increment, residual, direction, wind_u, wind_v, diffusion, vertical, background_inv,
    side_pair, side_flip, obs_column, obs_time, obs_count, jacobian, error_inv,
):
    sizes = grid_sizes()
    tiles, levs, subs = sizes
    panels = tiles * subs
    everyone = panels * levs
    width = increment.shape[2]
    slots, _, channels = jacobian.shape
    half = width // levs
    rows = half + MARGIN
    dma = pltpu.SemaphoreType.DMA
    inputs = (
        direction, wind_u, wind_v, obs_column[None, :], obs_time[None, :], obs_count,
        jacobian.reshape(slots, channels), error_inv, side_pair.T, side_flip.T, diffusion, vertical,
        background_inv, residual,
    )
    scalars = (5, 8, 9, 10, 11, 12)
    landing = [
        (pltpu.SMEM if k in scalars else pltpu.VMEM)(x.shape, x.dtype) for k, x in enumerate(inputs)
    ]
    row = jax.ShapeDtypeStruct((1, 1, width), F32)
    image, alpha, beta = pl.pallas_call(
        functools.partial(whole_kernel, sizes, slot_capacity(slots, panels)),
        out_shape=(jax.ShapeDtypeStruct(increment.shape, F32), row, row),
        in_specs=[pl.BlockSpec(memory_space=pl.ANY)] * len(inputs),
        out_specs=(VM, VM, VM),
        scratch_shapes=landing + [
            dma((len(inputs),)),
            pltpu.VMEM((3, width, width), F32),
            pltpu.VMEM((levs, 3, rows, width), F32),
            pltpu.VMEM((levs, panels, 12 * STEPS + FACTS, width), F32),
            pltpu.VMEM((slots, channels), F32),
            pltpu.VMEM((slots // levs, channels), F32),
            pltpu.VMEM((levs, panels, 2, width), F32),
            pltpu.VMEM((levs, panels, levs, width), F32),
            pltpu.VMEM((everyone, 4, width), F32),
            pltpu.VMEM((half, width), F32),
            pltpu.VMEM((half, width), F32),
            pltpu.VMEM((half, width), F32),
            pltpu.VMEM((2, 2 * levs * 4 * panels, width), F32),
            pltpu.VMEM((FACTS, panels, width), F32),
            pltpu.VMEM((slots, width), F32),
            dma, dma,
            dma((tiles,)), dma((tiles,)),
            dma((tiles,)), dma((tiles,)),
            dma((subs, levs, tiles)), dma((subs, levs, tiles)),
            dma, dma,
            dma, dma,
            dma, dma,
            dma((everyone,)), dma((everyone,)),
            dma((everyone,)), dma((everyone,)),
            dma((everyone,)), dma((everyone,)),
        ],
        compiler_params=pltpu.CompilerParams(
            collective_id=0, has_side_effects=True, vmem_limit_bytes=16 * 1024 * 1024),
        name="whole",
    )(*[x if x.size == 1 else pltpu.with_memory_space_constraint(x, pltpu.HBM) for x in inputs])
    left = residual - alpha * image
    return increment + alpha * direction, left, left + beta * direction


def chosen(*args):
    tiles, levs, subs = grid_sizes()
    increment, jacobian = args[0], args[13]
    width, slots, panels = increment.shape[2], jacobian.shape[0], tiles * subs
    fits = (
        levs == 2
        and increment.shape[0] == 1
        and increment.shape[1] == width
        and panels * slot_capacity(slots, panels) == width
        and panels == 8
        and slots % (8 * levs) == 0
        and width % (8 * levs) == 0
        and STEPS <= MARGIN
        and width >= 2 * STEPS
    )
    return fused_body(*args) if fits else body(*args)


def solution(mesh):
    placed = (
        P(("member", "lev"), ("tile", "sub"), None),
        P(("member", "lev"), ("tile", "sub"), None),
        P(("member", "lev"), ("tile", "sub"), None),
        P(("member", "lev"), ("tile", "sub"), None),
        P(("member", "lev"), ("tile", "sub"), None),
        P(),
        P(),
        P(),
        P(),
        P(),
        P(("tile", "sub")),
        P(("tile", "sub")),
        P(("tile", "sub")),
        P(("tile", "sub"), "lev", None),
        P(),
    )
    return jax.shard_map(
        chosen,
        mesh=mesh,
        in_specs=placed,
        out_specs=(
            P(("member", "lev"), ("tile", "sub"), None),
            P(("member", "lev"), ("tile", "sub"), None),
            P(("member", "lev"), ("tile", "sub"), None),
        ),
        check_vma=False,
    )
```

```python
import jax
import jax.numpy as jnp
from jax import lax
from jax.experimental import pallas as pl
from jax.experimental.pallas import tpu as pltpu
import functools
from jax.sharding import PartitionSpec as P

STEPS = 4


def with_halo(block, sides, width):
    for axis, dim in sides:
        count = lax.axis_size(axis)
        forward = [(i, i + 1) for i in range(count - 1)]
        backward = [(target, source) for source, target in forward]
        low = lax.ppermute(
            lax.slice_in_dim(block, block.shape[dim] - width, None, axis=dim), axis, forward
        )
        high = lax.ppermute(lax.slice_in_dim(block, 0, width, axis=dim), axis, backward)
        block = jnp.concatenate([low, block, high], axis=dim)
    return block


def neighbours(strips, pair_rows, flip_rows):
    everyone = lax.all_gather(strips, ("tile", "sub"), axis=0, tiled=True)
    picked = everyone[pair_rows]
    return jnp.where(flip_rows[:, None, None] == 1, picked[:, :, ::-1], picked)


def level_padded(field):
    return with_halo(field, (("lev", 0),), 1)


def body(
    increment,
    residual,
    direction,
    wind_u,
    wind_v,
    diffusion,
    vertical,
    background_inv,
    side_pair,
    side_flip,
    obs_column,
    obs_time,
    obs_count,
    jacobian,
    error_inv,
):
    depth = increment.shape[0]
    width = increment.shape[2]
    slots = obs_column.shape[0]
    panels = lax.axis_size(("tile", "sub"))
    capacity = max(2, (2 * slots + panels - 1) // panels)
    panel = lax.axis_index(("tile", "sub"))
    first_level = lax.axis_index("lev") * depth
    mixing = lax.dynamic_slice_in_dim(diffusion, first_level, depth)[:, None, None]
    blending = lax.dynamic_slice_in_dim(vertical, first_level, depth)[:, None, None]
    prior = lax.dynamic_slice_in_dim(background_inv, first_level, depth)[:, None, None]
    pair_rows = lax.dynamic_index_in_dim(side_pair, panel, 0, keepdims=False)
    flip_rows = lax.dynamic_index_in_dim(side_flip, panel, 0, keepdims=False)
    speed_u = wind_u.astype(jnp.float32)
    speed_v = wind_v.astype(jnp.float32)
    coefs = (
        mixing + 0.5 * speed_u,
        mixing - 0.5 * speed_u,
        mixing + 0.5 * speed_v,
        mixing - 0.5 * speed_v,
    )
    center = 1.0 - 4.0 * mixing - 2.0 * blending

    def forward(field):
        strips = jnp.stack([field[:, 0, :], field[:, -1, :], field[:, :, 0], field[:, :, -1]])
        halos = neighbours(strips, pair_rows, flip_rows)
        north = jnp.concatenate([halos[0][:, None, :], field[:, :-1, :]], axis=1)
        south = jnp.concatenate([field[:, 1:, :], halos[1][:, None, :]], axis=1)
        west = jnp.concatenate([halos[2][:, :, None], field[:, :, :-1]], axis=2)
        east = jnp.concatenate([field[:, :, 1:], halos[3][:, :, None]], axis=2)
        padded = level_padded(field)
        return (
            center * field
            + coefs[0] * north
            + coefs[1] * south
            + coefs[2] * west
            + coefs[3] * east
            + blending * (padded[:-2] + padded[2:])
        )

    def adjoint(field):
        prods = [c * field for c in coefs]
        strips = jnp.stack(
            [prods[0][:, 0, :], prods[1][:, -1, :], prods[2][:, :, 0], prods[3][:, :, -1]]
        )
        halos = neighbours(strips, pair_rows, flip_rows)
        rows_term = jnp.concatenate([prods[0][:, 1:, :], halos[1][:, None, :]], axis=1)
        rows_term = rows_term + jnp.concatenate([halos[0][:, None, :], prods[1][:, :-1, :]], axis=1)
        cols_term = jnp.concatenate([prods[2][:, :, 1:], halos[3][:, :, None]], axis=2)
        cols_term = cols_term + jnp.concatenate([halos[2][:, :, None], prods[3][:, :, :-1]], axis=2)
        padded = level_padded(blending * field)
        return center * field + rows_term + cols_term + padded[:-2] + padded[2:]

    state = direction
    states = []
    for step in range(STEPS):
        state = forward(state)
        states.append(state.reshape(depth, width * width))
    history = jnp.stack(states, axis=0)
    area = width * width
    alive = jnp.arange(slots, dtype=jnp.int32) < obs_count[0]
    targets = obs_column // area
    cells = obs_column % area
    owned = (
        (targets[:, None] == jnp.arange(panels, dtype=jnp.int32)[None, :]) & alive[:, None]
    ).astype(jnp.int32)
    rank = jnp.sum((jnp.cumsum(owned, axis=0) - owned) * owned, axis=1)
    position = jnp.where(alive, targets * capacity + rank, panels * capacity)
    want_cell = (
        jnp.zeros((panels * capacity,), jnp.int32)
        .at[position]
        .set(cells, mode="drop")
        .reshape(panels, capacity)
    )
    want_time = (
        jnp.ones((panels * capacity,), jnp.int32)
        .at[position]
        .set(obs_time, mode="drop")
        .reshape(panels, capacity)
    )
    asked_cell = lax.all_to_all(want_cell, ("tile", "sub"), split_axis=0, concat_axis=0, tiled=True)
    asked_time = lax.all_to_all(want_time, ("tile", "sub"), split_axis=0, concat_axis=0, tiled=True)
    values = history[asked_time - 1, :, asked_cell]
    sent = lax.all_to_all(values, ("tile", "sub"), split_axis=0, concat_axis=0, tiled=True)
    gathered = sent.reshape(panels * capacity, depth)[jnp.minimum(position, panels * capacity - 1)]
    wide = jacobian.astype(jnp.float32)
    partial_value = jnp.einsum("olc,ol->oc", wide, gathered, precision=lax.Precision.HIGHEST)
    departure = lax.psum(partial_value, "lev")
    weighted = departure * error_inv[None, :]
    back = jnp.einsum("olc,oc->ol", wide, weighted, precision=lax.Precision.HIGHEST)
    back = back * alive.astype(jnp.float32)[:, None]
    outgoing = (
        jnp.zeros((panels * capacity, depth), jnp.float32)
        .at[position]
        .set(back, mode="drop")
        .reshape(panels, capacity, depth)
    )
    incoming = lax.all_to_all(outgoing, ("tile", "sub"), split_axis=0, concat_axis=0, tiled=True)
    flat_cell = asked_cell.reshape(panels * capacity)
    flat_time = asked_time.reshape(panels * capacity) - 1
    forcing = (
        jnp.zeros((STEPS, depth, area), jnp.float32)
        .at[flat_time, :, flat_cell]
        .add(incoming.reshape(panels * capacity, depth))
    )
    forcing = forcing.reshape(STEPS, depth, width, width)
    sensitivity = forcing[STEPS - 1]
    for step in range(STEPS - 1, 0, -1):
        sensitivity = adjoint(sensitivity) + forcing[step - 1]
    sensitivity = adjoint(sensitivity)
    image = prior * direction + sensitivity
    norm_old, curvature, cross, square = lax.psum(
        (
            jnp.sum(residual * residual),
            jnp.sum(direction * image),
            jnp.sum(residual * image),
            jnp.sum(image * image),
        ),
        ("tile", "lev", "sub"),
    )
    alpha = norm_old / curvature
    increment_new = increment + alpha * direction
    residual_new = residual - alpha * image
    norm_new = norm_old - 2.0 * alpha * cross + alpha * alpha * square
    direction_new = residual_new + norm_new / norm_old * direction
    return (increment_new, residual_new, direction_new)


MESH = pl.DeviceIdType.MESH
VM = pl.BlockSpec(memory_space=pltpu.VMEM)
F32 = jnp.float32
BF16 = jnp.bfloat16
NT = (((1,), (1,)), ((), ()))
TN = (((0,), (0,)), ((), ()))
NN = (((1,), (0,)), ((), ()))
FACTS = 3
MARGIN = 8
INPUTS = 14


def grid_sizes():
    return lax.axis_size("tile"), lax.axis_size("lev"), lax.axis_size("sub")


def slot_capacity(slots, panels):
    return max(2, (2 * slots + panels - 1) // panels)


def hail(peers):
    barrier = pltpu.get_barrier_semaphore()
    for peer in peers:
        pl.semaphore_signal(barrier, inc=1, device_id=peer, device_id_type=MESH)


def hailed(peers):
    pl.semaphore_wait(pltpu.get_barrier_semaphore(), len(peers))


def group_peers(sizes):
    axes = ("tile", "lev", "sub")
    steps = [(t, l, u) for t in range(sizes[0]) for l in range(sizes[1]) for u in range(sizes[2])]
    steps.sort(key=lambda d: (-min(d[0], sizes[0] - d[0]), -d[1], -d[2]))
    return [
        {axis: lax.rem(lax.axis_index(axis) + by, size) for axis, by, size in zip(axes, d, sizes)}
        for d in steps if any(d)
    ]


def by_distance(tile, tiles):
    table = [sorted((t for t in range(tiles) if t != me), key=lambda t: abs(t - me)) for me in range(tiles)]
    picks = []
    for k in range(tiles - 1):
        pick = jnp.int32(table[0][k])
        for me in range(1, tiles):
            pick = jnp.where(tile == me, table[me][k], pick)
        picks.append(pick)
    return picks


def dot(a, b, dims, precision=None):
    return lax.dot_general(a, b, dims, precision=precision, preferred_element_type=F32)


def iota(shape, axis):
    return lax.broadcasted_iota(jnp.int32, shape, axis)


def fiota(shape, axis):
    return iota(shape, axis).astype(F32)


def halves(x):
    high = x.astype(BF16).astype(F32)
    return high, x - high


def per_level(ref, levels, ndim):
    return jnp.stack([jnp.full((1,) * (ndim - 1), ref[l], F32) for l in range(levels)])


def edge_index(shape, rows, width):
    r = iota(shape, len(shape) - 2)
    return jnp.where(r < rows // 2, r, r + (width - rows))


def column_of(halo, hit):
    return jnp.sum(jnp.where(hit, halo, 0.0), axis=-1, keepdims=True)


def shifted(x, axis, by, edge):
    n = x.shape[axis]
    rolled = pltpu.roll(x, by % n, axis)
    place_of = iota(x.shape[-2:], axis - (x.ndim - 2))
    return jnp.where(place_of == (0 if by == 1 else n - 1), edge, rolled)


def vertical_sum(x):
    levels = x.shape[0]
    parts = []
    for l in range(levels):
        total = jnp.zeros_like(x[l])
        if l > 0:
            total = total + x[l - 1]
        if l + 1 < levels:
            total = total + x[l + 1]
        parts.append(total)
    return jnp.stack(parts)


def forward_tile(x, c, center, vert, h, hit):
    r, w = x.ndim - 2, x.ndim - 1
    return (
        center * x
        + c[0] * shifted(x, r, 1, h[0])
        + c[1] * shifted(x, r, -1, h[1])
        + c[2] * shifted(x, w, 1, column_of(h[2], hit))
        + c[3] * shifted(x, w, -1, column_of(h[3], hit))
        + vert * vertical_sum(x)
    )


def adjoint_tile(x, p, center, vert, h, hit):
    r, w = x.ndim - 2, x.ndim - 1
    return (
        center * x
        + shifted(p[0], r, -1, h[1])
        + shifted(p[1], r, 1, h[0])
        + shifted(p[2], w, -1, column_of(h[3], hit))
        + shifted(p[3], w, 1, column_of(h[2], hit))
        + vertical_sum(vert * x)
    )


def swap(q):
    return (q[2], q[3], q[0], q[1])


def turned(x):
    width = x.shape[1]
    back = width - 1 - iota((8, width), 1)
    return jnp.concatenate(
        [jnp.take_along_axis(x[r : r + 8], back, axis=1) for r in range(0, x.shape[0], 8)], axis=0)


def partner_rows(pair_ref, flip_ref, levels, panels):
    sides = 4 * panels

    def row(k, p):
        pair = pair_ref[k, p]
        return (flip_ref[k, p] * levels * sides) + (pair % 4) * panels + pair // 4

    return row


def exchange(strips, store, row, panel):
    levels, panels, _, width = strips[0].shape
    sides = 4 * panels
    s = jnp.concatenate(
        [strips[k][l].reshape(panels, width) for l in range(levels) for k in range(4)], axis=0)
    store[: levels * sides] = s
    store[levels * sides :] = turned(s)

    def strip(k, p, l):
        return store[pl.ds(row(k, p) + l * sides, 1), :]

    every = [
        jnp.stack([jnp.stack([strip(k, p, l) for p in range(panels)]) for l in range(levels)])
        for k in range(4)
    ]
    return every, [jnp.stack([strip(k, panel, l) for l in range(levels)]) for k in range(4)]


def slot_rows(col, when, count, panels, area, width, capacity):
    slots = col.shape[1]
    alive = iota((1, slots), 1) < count
    panel = jnp.where(alive, col // area, -1)
    cell = col % area
    owned = (iota((panels, slots), 0) == panel).astype(F32)
    earlier = (iota((slots, slots), 0) < iota((slots, slots), 1)).astype(BF16)
    rank = jnp.sum(owned * dot(owned.astype(BF16), earlier, NN), axis=0, keepdims=True)
    slot = jnp.where(alive, panel.astype(F32) * capacity + rank, -1.0)
    spread = (fiota((panels * capacity, slots), 0) == slot).astype(BF16)
    facts = jnp.concatenate([cell // width + 1, cell % width + 1, when], axis=0).astype(F32)
    facts = jnp.concatenate([facts, jnp.zeros((8 - FACTS, slots), F32)], axis=0)
    tall = jnp.concatenate([slot, jnp.zeros((7, slots), F32)], axis=0).T
    upright = (fiota((slots, panels * capacity), 1) == tall[:, 0:1]).astype(F32)
    return dot(facts.astype(BF16), spread, NT), spread, upright


def by_panel(a, capacity):
    owners, width = a.shape
    mine = iota((owners, width), 1) // capacity == iota((owners, width), 0)
    slanted = pltpu.roll(a, 0, 1, stride=capacity, stride_axis=0)
    rows = []
    for p in range(width // capacity):
        r = pltpu.roll(slanted, width - p * capacity, 1) if p else slanted
        rows.append(jnp.sum(jnp.where(mine, r, 0.0), axis=0, keepdims=True))
    return jnp.concatenate(rows, axis=0)


def whole_kernel(sizes, capacity, *refs):
    tiles, levs, subs = sizes
    inputs, (img_out, alpha_out, beta_out) = refs[:INPUTS], refs[INPUTS : INPUTS + 3]
    held = refs[INPUTS + 3 : 2 * INPUTS + 3]
    (landed, stage, win, bands, jmine, jother, gall, vall, sall, rother, isent, igot, store, box, upright,
     fsend, frecv, zsend, zrecv, xsend, xrecv, csend, crecv, jsend, jrecv, rsend, rrecv, isend, irecv,
     gsend, grecv, vsend, vrecv, ssend, srecv) = refs[2 * INPUTS + 3 :]
    (dir_ref, wu_ref, wv_ref, col_ref, time_ref, count_ref, jac_ref, err_ref, pair_ref, flip_ref,
     dif_ref, ver_ref, inv_ref, res_ref) = held
    loads = [
        pltpu.make_async_copy(src, dst, landed.at[k]) for k, (src, dst) in enumerate(zip(inputs, held))
    ]
    flat_peers = group_peers(sizes)
    near = [{axis: lax.rem(lax.axis_index(axis) + k, size)}
            for axis, size in zip(("tile", "lev", "sub"), sizes) for k in range(1, size)]
    hail(near)
    for load in loads[:6]:
        load.start()
    for load in loads[6:]:
        load.start()

    tile, lev, sub = lax.axis_index("tile"), lax.axis_index("lev"), lax.axis_index("sub")
    panels = tiles * subs
    panel = tile * subs + sub
    me = (tile * levs + lev) * subs + sub
    other = 1 - lev
    slots, channels = jac_ref.shape
    width = dir_ref.shape[2]
    area = width * width
    tips = 2 * STEPS
    last = tips - 1
    base = 6 * tips
    half = width // levs
    rows = half + MARGIN
    start = pl.multiple_of(lev * (width - rows), MARGIN)
    ostart = pl.multiple_of(other * (width - rows), MARGIN)
    mid = pl.multiple_of(lev * half, MARGIN)
    omid = pl.multiple_of(other * half, MARGIN)
    share = slots // levs

    for f, ref in enumerate((dir_ref, wu_ref, wv_ref)):
        loads[f].wait()
        x = ref[0].astype(F32)
        stage[f] = x
        xt = x.T
        at = 2 * tips * f
        bands[lev, panel, at : at + STEPS] = x[:STEPS]
        bands[lev, panel, at + STEPS : at + tips] = x[width - STEPS :]
        bands[lev, panel, at + tips : at + tips + STEPS] = xt[:STEPS]
        bands[lev, panel, at + tips + STEPS : at + 2 * tips] = xt[width - STEPS :]
    for load in loads[3:6]:
        load.wait()
    facts, spread, upright[...] = slot_rows(
        col_ref[...], time_ref[...], count_ref[0], panels, area, width, capacity)
    bands[lev, panel, base : base + FACTS] = facts[:FACTS]
    hailed(near)
    started = []

    def remote(src, dst, ssem, rsem, where):
        return pltpu.make_async_remote_copy(
            src_ref=src, dst_ref=dst, send_sem=ssem, recv_sem=rsem,
            device_id=where, device_id_type=MESH)

    def send(src, dst, ssem, rsem, where):
        copy = remote(src, dst, ssem, rsem, where)
        copy.start()
        started.append(copy)
        return copy

    def block(level, at, by=0):
        index = at * subs + lax.rem(sub + by, subs)
        return bands.at[level, index] if level is lev else bands.at[level, index, pl.ds(0, base)]

    def across_block(level, at):
        return bands.at[level, at * subs + sub, pl.ds(0, base)]

    arrivals_x, arrivals_c = [], []
    across = {"lev": other}

    def to_subs(level, at, k):
        for q in range(1, subs):
            arrivals_c.append(send(block(level, at), block(level, at), csend.at[q, level, k], crecv.at[q, level, at],
                                   {"sub": lax.rem(sub + q, subs)}))

    def to_lev(at, k):
        arrivals_x.append(send(across_block(lev, at), across_block(lev, at), xsend.at[k], xrecv.at[at], across))

    order = by_distance(tile, tiles)
    sends = list(enumerate(order))[::-1]
    for k, at in sends:
        send(block(lev, tile), block(lev, tile), zsend.at[k], zrecv.at[tile], {"tile": at})
    to_lev(tile, 0)
    to_subs(lev, tile, 0)
    fields = send(stage.at[:, pl.ds(ostart, rows)], win.at[lev], fsend, frecv, across)
    for f in range(3):
        win[lev, f] = stage[f, pl.ds(start, rows)]
    for load in loads[6:]:
        load.wait()
    jmine[...] = jac_ref[...].astype(F32)
    partner = partner_rows(pair_ref, flip_ref, levs, panels)
    e8 = jnp.broadcast_to(err_ref[...][None, :], (8, channels))
    high = lax.Precision.HIGHEST

    def slotted(g):
        a, b = halves(g)
        both = jnp.concatenate([a, b], axis=0).astype(BF16)
        out = dot(both, spread, NT)
        return out[:1] + out[8:9]

    gall[lev, panel, 0:1] = slotted(dot(e8, jmine[...] * jmine[...], NT, high))
    for k, at in enumerate(order):
        remote(block(lev, at), block(lev, at), zsend.at[k], zrecv.at[at], {"tile": at}).wait_recv()
        to_lev(at, k + 1)
        to_subs(lev, at, k + 1)

    def from_sub(level):
        for q in range(1, subs):
            for at in [tile] + order:
                whence = block(level, at, q)
                remote(whence, whence, csend.at[q, level, 0], crecv.at[q, level, at],
                       {"sub": lax.rem(sub + q, subs)}).wait_recv()

    from_sub(lev)
    jcopy = send(jmine.at[pl.ds(pl.multiple_of(other * share, MARGIN), share)], jother, jsend, jrecv, across)
    for k, at in enumerate([tile] + order):
        remote(across_block(other, at), across_block(other, at), xsend.at[k], xrecv.at[at], across).wait_recv()
        to_subs(other, at, k)

    o_i, o_j, o_t = [by_panel(bands[lev, :, base + k, :], capacity) for k in range(FACTS)]
    for k, v in enumerate((o_i, o_j, o_t)):
        box[k] = v
    s_i, s_j, s_t = [box[k, pl.ds(panel, 1), :] for k in range(FACTS)]
    line = iota((rows, width), 0)
    mine = (line + start + 1).astype(F32) == s_i
    inside = jnp.where((line >= lev * MARGIN) & (line < lev * MARGIN + half), 1.0, 0.0)
    here = jnp.where(mine, inside, 0.0)
    fields.wait_recv()
    from_sub(other)

    def band(f, which):
        at = (2 * f + which) * tips
        return bands[:, :, at : at + tips, :]

    def coefs(m, u, v):
        return (m + 0.5 * u, m - 0.5 * u, m + 0.5 * v, m - 0.5 * v)

    m4, v4 = per_level(dif_ref, levs, 4), per_level(ver_ref, levs, 4)
    m3, v3 = per_level(dif_ref, levs, 3), per_level(ver_ref, levs, 3)
    ns = coefs(m4, band(1, 0), band(2, 0))
    we = swap(coefs(m4, band(1, 1), band(2, 1)))
    own = coefs(m3, win[:, 1], win[:, 2])
    scal4 = (1.0 - 4.0 * m4 - 2.0 * v4, v4)
    scal3 = (1.0 - 4.0 * m3 - 2.0 * v3, v3)
    hit4 = edge_index((tips, width), tips, width) == iota((tips, width), 1)
    hit3 = iota((rows, width), 0) + start == iota((rows, width), 1)
    x_ns, x_we, x = band(0, 0), band(0, 1), win[:, 0]

    at_j = fiota((width, width), 0) + 1.0 == s_j
    pick_j = jnp.where(at_j, 1.0, 0.0)
    pick_j = jnp.concatenate([pick_j, pick_j], axis=0).astype(BF16)
    picked = jnp.zeros((levs, rows, width), F32)
    for step in range(STEPS):
        strips = (x_ns[:, :, :1], x_ns[:, :, last:], x_we[:, :, :1], x_we[:, :, last:])
        h, ho = exchange(strips, store.at[step % 2], partner, panel)
        x = forward_tile(x, own, *scal3, ho, hit3)
        if step + 1 < STEPS:
            x_ns, x_we = (
                forward_tile(x_ns, ns, *scal4, h, hit4),
                forward_tile(x_we, we, *scal4, swap(h), hit4),
            )
        now = jnp.where(s_t == step + 1.0, here, 0.0)
        both = jnp.concatenate([jnp.concatenate(halves(x[l]), axis=1) for l in range(levs)], axis=0)
        picked = picked + now * dot(both.astype(BF16), pick_j, NN).reshape(levs, rows, width)
        if step == 2:
            jcopy.wait_recv()
            near_half = pl.multiple_of(lev * share, MARGIN)
            cross = jmine[pl.ds(near_half, share)] * jother[...] * err_ref[...][None, :]
            cross = jnp.sum(cross, axis=1, keepdims=True) * upright[pl.ds(near_half, share)]
            gall[lev, panel, 1:2] = jnp.sum(cross, axis=0, keepdims=True)
            arrivals_g = [
                send(gall.at[lev, panel], gall.at[lev, panel], gsend.at[k], grecv.at[k], where)
                for k, where in enumerate(flat_peers)
            ]
    for l in range(levs):
        vall[lev, panel, l : l + 1] = jnp.sum(picked[l], axis=0, keepdims=True)
    arrivals_v = [
        send(vall.at[lev, panel], vall.at[lev, panel], vsend.at[k], vrecv.at[k], where)
        for k, where in enumerate(flat_peers)
    ]

    rcopy = send(res_ref.at[0, pl.ds(omid, half)], rother, rsend, rrecv, across)
    edge = edge_index((tips, width), tips, width).astype(F32) + 1.0
    spots = fiota((width, width), 0) + 1.0

    def onehots(p, a, b):
        tip = jnp.concatenate(
            [jnp.where((edge == a[p : p + 1]) & (o_t[p : p + 1] == t), 1.0, 0.0)
             for t in range(1, STEPS + 1)], axis=0)
        along = jnp.where(spots == b[p : p + 1], 1.0, 0.0)
        return tip, jnp.concatenate([along, along], axis=1).astype(BF16)

    hot_ns = [onehots(p, o_i, o_j) for p in range(panels)]
    hot_we = [onehots(p, o_j, o_i) for p in range(panels)]
    rows_own = jnp.concatenate(
        [jnp.where(mine & (s_t == t), 1.0, 0.0) for t in range(1, STEPS + 1)], axis=0)
    rows_own = jnp.concatenate([rows_own, rows_own], axis=1).astype(BF16)
    for copy in arrivals_g:
        copy.wait_recv()
    gram = {(l, l): by_panel(gall[l, :, 0, :], capacity) for l in range(levs)}
    gram[0, 1] = gram[1, 0] = by_panel(gall[0, :, 1, :] + gall[1, :, 1, :], capacity)
    for copy in arrivals_v:
        copy.wait_recv()
    total = vall[0] + vall[1]
    back = [gram[a, 0] * total[:, 0] + gram[a, 1] * total[:, 1] for a in range(levs)]
    parts = [halves(b) for b in back]

    def band_forcing(hot):
        out = []
        for p in range(panels):
            tip, along = hot[p]
            left = jnp.concatenate(
                [jnp.concatenate([tip * v[p : p + 1] for v in parts[l]], axis=1) for l in range(levs)],
                axis=0)
            out.append(dot(left.astype(BF16), along, NT))
        return [
            jnp.stack([
                jnp.stack([o[(l * STEPS + t) * tips : (l * STEPS + t + 1) * tips] for o in out])
                for l in range(levs)])
            for t in range(STEPS)
        ]

    for l in range(levs):
        box[l] = back[l]
    scaled = []
    for l in range(levs):
        v = halves(box[l, pl.ds(panel, 1), :])
        scaled.append(jnp.concatenate([jnp.where(at_j, w, 0.0) for w in v], axis=1))
    flat = dot(rows_own, jnp.concatenate(scaled, axis=0).astype(BF16), NT)
    force = [
        jnp.stack([flat[t * rows : (t + 1) * rows, l * width : (l + 1) * width] for l in range(levs)])
        for t in range(STEPS)
    ]
    force_ns, force_we = band_forcing(hot_ns), band_forcing(hot_we)
    x, x_ns, x_we = force[-1], force_ns[-1], force_we[-1]
    for step in range(STEPS - 1, -1, -1):
        p_ns = [c * x_ns for c in ns]
        p_we = [c * x_we for c in we]
        strips = (p_ns[0][:, :, :1], p_ns[1][:, :, last:], p_we[0][:, :, :1], p_we[1][:, :, last:])
        h, ho = exchange(strips, store.at[step % 2], partner, panel)
        x = adjoint_tile(x, [c * x for c in own], *scal3, ho, hit3)
        if step > 0:
            x = x + force[step - 1]
            x_ns = adjoint_tile(x_ns, p_ns, *scal4, h, hit4) + force_ns[step - 1]
            x_we = adjoint_tile(x_we, p_we, *scal4, swap(h), hit4) + force_we[step - 1]

    rcopy.wait_recv()
    x = jnp.where(lev == 0, x[:, :half], x[:, rows - half :])
    direction = [win[l, 0, pl.ds(pl.multiple_of(lev * MARGIN, MARGIN), half)] for l in range(levs)]
    image = [x[l] + inv_ref[l] * direction[l] for l in range(levs)]
    own_res, other_res = res_ref[0, pl.ds(mid, half)], rother[...]
    sums = None
    for l in range(levs):
        res = jnp.where(lev == l, own_res, other_res)
        pairs = ((res, res), (direction[l], image[l]), (res, image[l]), (image[l], image[l]))
        part = jnp.concatenate([jnp.sum(a * b, axis=0, keepdims=True) for a, b in pairs], axis=0)
        sums = part if sums is None else sums + part
    sall[me] = sums
    before = list(started)
    arrivals_s = [
        send(sall.at[me], sall.at[me], ssend.at[k], srecv.at[k], where)
        for k, where in enumerate(flat_peers)
    ]
    isent[...] = jnp.where(lev == 0, image[1], image[0])
    icopy = send(isent, igot, isend, irecv, across)
    img_out[0, pl.ds(mid, half)] = jnp.where(lev == 0, image[0], image[1])
    for copy in before:
        copy.wait_send()
    icopy.wait_recv()
    img_out[0, pl.ds(omid, half)] = igot[...]
    for copy in arrivals_s:
        copy.wait_recv()
    total = jnp.sum(jnp.sum(sall[...], axis=0), axis=1, keepdims=True)
    old, curvature, cross, square = [total[k : k + 1] for k in range(4)]
    alpha = old / curvature
    new = old - 2.0 * alpha * cross + alpha * alpha * square
    alpha_out[0] = jnp.broadcast_to(alpha, alpha_out.shape[1:])
    beta_out[0] = jnp.broadcast_to(new / old, beta_out.shape[1:])
    for copy in started[len(before) :]:
        copy.wait_send()


def fused_body(
    increment, residual, direction, wind_u, wind_v, diffusion, vertical, background_inv,
    side_pair, side_flip, obs_column, obs_time, obs_count, jacobian, error_inv,
):
    sizes = grid_sizes()
    tiles, levs, subs = sizes
    panels = tiles * subs
    everyone = panels * levs
    width = increment.shape[2]
    slots, _, channels = jacobian.shape
    half = width // levs
    rows = half + MARGIN
    dma = pltpu.SemaphoreType.DMA
    inputs = (
        direction, wind_u, wind_v, obs_column[None, :], obs_time[None, :], obs_count,
        jacobian.reshape(slots, channels), error_inv, side_pair.T, side_flip.T, diffusion, vertical,
        background_inv, residual,
    )
    scalars = (5, 8, 9, 10, 11, 12)
    landing = [
        (pltpu.SMEM if k in scalars else pltpu.VMEM)(x.shape, x.dtype) for k, x in enumerate(inputs)
    ]
    row = jax.ShapeDtypeStruct((1, 1, width), F32)
    image, alpha, beta = pl.pallas_call(
        functools.partial(whole_kernel, sizes, slot_capacity(slots, panels)),
        out_shape=(jax.ShapeDtypeStruct(increment.shape, F32), row, row),
        in_specs=[pl.BlockSpec(memory_space=pl.ANY)] * len(inputs),
        out_specs=(VM, VM, VM),
        scratch_shapes=landing + [
            dma((len(inputs),)),
            pltpu.VMEM((3, width, width), F32),
            pltpu.VMEM((levs, 3, rows, width), F32),
            pltpu.VMEM((levs, panels, 12 * STEPS + FACTS, width), F32),
            pltpu.VMEM((slots, channels), F32),
            pltpu.VMEM((slots // levs, channels), F32),
            pltpu.VMEM((levs, panels, 2, width), F32),
            pltpu.VMEM((levs, panels, levs, width), F32),
            pltpu.VMEM((everyone, 4, width), F32),
            pltpu.VMEM((half, width), F32),
            pltpu.VMEM((half, width), F32),
            pltpu.VMEM((half, width), F32),
            pltpu.VMEM((2, 2 * levs * 4 * panels, width), F32),
            pltpu.VMEM((FACTS, panels, width), F32),
            pltpu.VMEM((slots, width), F32),
            dma, dma,
            dma((tiles,)), dma((tiles,)),
            dma((tiles,)), dma((tiles,)),
            dma((subs, levs, tiles)), dma((subs, levs, tiles)),
            dma, dma,
            dma, dma,
            dma, dma,
            dma((everyone,)), dma((everyone,)),
            dma((everyone,)), dma((everyone,)),
            dma((everyone,)), dma((everyone,)),
        ],
        compiler_params=pltpu.CompilerParams(
            collective_id=0, has_side_effects=True, vmem_limit_bytes=16 * 1024 * 1024),
        name="whole",
    )(*[x if x.size == 1 else pltpu.with_memory_space_constraint(x, pltpu.HBM) for x in inputs])
    left = residual - alpha * image
    return increment + alpha * direction, left, left + beta * direction


def chosen(*args):
    tiles, levs, subs = grid_sizes()
    increment, jacobian = args[0], args[13]
    width, slots, panels = increment.shape[2], jacobian.shape[0], tiles * subs
    fits = (
        levs == 2
        and increment.shape[0] == 1
        and increment.shape[1] == width
        and panels * slot_capacity(slots, panels) == width
        and panels == 8
        and slots % (8 * levs) == 0
        and width % (8 * levs) == 0
        and STEPS <= MARGIN
        and width >= 2 * STEPS
    )
    return fused_body(*args) if fits else body(*args)


def solution(mesh):
    placed = (
        P(("member", "lev"), ("tile", "sub"), None),
        P(("member", "lev"), ("tile", "sub"), None),
        P(("member", "lev"), ("tile", "sub"), None),
        P(("member", "lev"), ("tile", "sub"), None),
        P(("member", "lev"), ("tile", "sub"), None),
        P(),
        P(),
        P(),
        P(),
        P(),
        P(("tile", "sub")),
        P(("tile", "sub")),
        P(("tile", "sub")),
        P(("tile", "sub"), "lev", None),
        P(),
    )
    return jax.shard_map(
        chosen,
        mesh=mesh,
        in_specs=placed,
        out_specs=(
            P(("member", "lev"), ("tile", "sub"), None),
            P(("member", "lev"), ("tile", "sub"), None),
            P(("member", "lev"), ("tile", "sub"), None),
        ),
        check_vma=False,
    )
```
